256 devices in a mesh: rep: 8 (over z_lo, x), pts: 32 (over y, z_hi, core).
Axes of the slice: x: 4, y: 4, z: 8 (z_hi: 4, z_lo: 2; z = z_hi * 2 + z_lo), core: 2. Of those that a mesh axis runs over, the one named last changes fastest.
Arguments:
- fine_points: bfloat16 [262144, 256], P(('rep', 'pts')), may hold values from -6 to 6
- parent: int32 [262144], P(('rep', 'pts')), may hold values from 0 to 65535, as said below
- patch_count: int32 [256], P(('rep', 'pts')), may hold values from 512 to 1024
- qkv_fine: bfloat16 [256, 768], replicated, may hold values from -0.375 to 0.375
- out_fine: bfloat16 [256, 256], replicated, may hold values from -0.375 to 0.375
- pool_weight: bfloat16 [256, 512], replicated, may hold values from -0.375 to 0.375
- qkv_coarse: bfloat16 [512, 1536], replicated, may hold values from -0.25 to 0.25
- out_coarse: bfloat16 [512, 512], replicated, may hold values from -0.25 to 0.25
- cotangent: bfloat16 [65536, 512], P(('rep', 'pts')), may hold values from -6 to 6
Outputs:
- coarse_out: bfloat16 [65536, 512], P(('rep', 'pts'))
- grad_out_fine: bfloat16 [256, 256], replicated
- grad_pool: bfloat16 [256, 512], replicated
- grad_qkv_coarse: bfloat16 [512, 1536], replicated
- grad_out_coarse: bfloat16 [512, 512], replicated
The draws below stay inside these ranges and needn't reach their ends.
Inputs may be any that keep to these rules, and one draw needn't show every extreme that they name: `parent`: along the points of block b, parents never fall and lie in pooled rows b * 256 to (b + 1) * 256 + 31; the last block of each replica (pts index 31) keeps its parents in its own 256 rows.
All inputs are finite; a program needn't handle non-finite values.
Results may differ from the reference program's by a relative error of at most 0.018.
Values may be sent and summed in bfloat16 or wider, within the bound.
A program may use at most 128 MiB of HBM per device.

```python
import jax
import jax.numpy as jnp
from jax import lax

C1 = 256
C2 = 512
HD = 16
PATCH = 1024
P_DEV = 1024
Q_DEV = 256
SPILL = 32
NP = 262144
NQ = 65536
NPATCH = 256
N_REP = 8
N_PTS = 32


def draw_parent(key, part):
    devices = N_REP * N_PTS
    reach = jnp.where(jnp.arange(devices) % N_PTS == N_PTS - 1, Q_DEV, Q_DEV + SPILL)
    raw_bits = jax.random.randint(jax.random.fold_in(key, 17), (devices, P_DEV), 0, 1 << 20)
    picker = jax.random.randint(jax.random.fold_in(key, 29), (devices, P_DEV), 0, 10)
    spilling = (picker < 3) & (reach > Q_DEV)[:, None]
    spill_pick = Q_DEV + raw_bits % SPILL
    spread_pick = raw_bits % reach[:, None]
    offsets = jnp.sort(jnp.where(spilling, spill_pick, spread_pick), axis=1)
    return (offsets + jnp.arange(devices)[:, None] * Q_DEV).reshape(-1).astype(jnp.int32)


def place_ends(values, rng, low, high):
    extent = values.shape
    index_at = [jax.random.randint(jax.random.fold_in(rng, axis), (), 0, extent[axis]) for axis in range(len(extent))]
    values = values.at[tuple(index_at)].set(low)
    longest = extent.index(max(extent))
    index_at[longest] = (index_at[longest] + 1) % extent[longest]
    return values.at[tuple(index_at)].set(high)


def block_scale(rng, shape, pieces, least, largest):
    def one(dim, parts):
        draws = jax.random.uniform(jax.random.fold_in(jax.random.fold_in(rng, 6), dim), (parts,), jnp.float32, least / len(pieces), largest / len(pieces))
        return jnp.repeat(jnp.exp(draws), shape[dim] // parts).reshape((-1,) + (1,) * (len(shape) - dim - 1))

    level = one(*pieces[0])
    for cut in pieces[1:]:
        level = level * one(*cut)
    return level


def normal_values(own_key, extent, spread, most, split=(), held_as=jnp.bfloat16):
    result = jax.random.normal(own_key, extent, jnp.float32) * spread
    if len(split) > 0:
        result = block_scale(own_key, extent, split, -0.22, 0.18) * result
    return jnp.clip(result, min=-most, max=most).astype(held_as)


def setup_inputs(seed: int = 0) -> dict:
    keys = jax.random.split(jax.random.key(seed), 10)
    return {
        "fine_points": normal_values(keys[0], (NP, C1), 1.0, 6.0, ((0, 256),)),
        "parent": draw_parent(jax.random.fold_in(keys[9], 71), 0),
        "patch_count": place_ends(jax.random.randint(keys[2], (NPATCH,), PATCH // 2, PATCH + 1), jax.random.fold_in(keys[2], 1), PATCH // 2, PATCH).astype(jnp.int32),
        "qkv_fine": normal_values(keys[3], (C1, 3 * C1), C1 ** -0.5, 0.375),
        "out_fine": normal_values(keys[4], (C1, C1), C1 ** -0.5, 0.375),
        "pool_weight": normal_values(keys[5], (C1, C2), C1 ** -0.5, 0.375),
        "qkv_coarse": normal_values(keys[6], (C2, 3 * C2), C2 ** -0.5, 0.25),
        "out_coarse": normal_values(keys[7], (C2, C2), C2 ** -0.5, 0.25),
        "cotangent": normal_values(keys[8], (NQ, C2), 1.0, 6.0, ((0, 256),)),
    }


epsilon = 1e-06
logit_scale = 0.25

def normalize(values):
    return values * lax.rsqrt(lax.optimization_barrier(jnp.mean(values * values, axis=-1, keepdims=True)) + epsilon)

def attend(queries, key_rows, value_rows, head_count, key_mask):
    query_rows = queries.shape[0]
    key_total = key_rows.shape[0]
    channels = queries.shape[1]
    head_size = channels // head_count
    group = min(4, head_count)
    groups = head_count // group
    head_query = queries.reshape(query_rows, groups, group, head_size).transpose(1, 0, 2, 3)
    head_key = key_rows.reshape(key_total, groups, group, head_size).transpose(1, 0, 2, 3)
    head_value = value_rows.reshape(key_total, groups, group, head_size).transpose(1, 0, 2, 3)

    @jax.checkpoint
    def one_group(element):
        grouped_query_rows, grouped_key_rows, grouped_value_rows = element
        logit_table = jnp.einsum('ygq,pgq->gyp', grouped_query_rows, grouped_key_rows, preferred_element_type=jnp.float32) * logit_scale
        if key_mask is not None:
            logit_table = jnp.where(key_mask[None, None, :], logit_table, -1e+30)
        logit_table = logit_table - lax.stop_gradient(lax.optimization_barrier(jnp.max(logit_table, axis=-1, keepdims=True)))
        exponent = jnp.exp(logit_table)
        attention_weight = (exponent / lax.optimization_barrier(jnp.sum(exponent, axis=-1, keepdims=True))).astype(jnp.bfloat16)
        grouped_mixture = jnp.einsum('yex,xyb->eyb', attention_weight, grouped_value_rows, preferred_element_type=jnp.float32)
        return grouped_mixture.astype(jnp.bfloat16)
    mixed_rows = lax.map(one_group, (head_query, head_key, head_value))
    return mixed_rows.transpose(1, 0, 2, 3).reshape(query_rows, channels)

def fine_attention(tokens, qkv_weight, patch_count):
    channels = tokens.shape[1]
    normed = normalize(tokens.astype(jnp.float32)).astype(jnp.bfloat16)
    packed = jnp.dot(normed, qkv_weight, preferred_element_type=jnp.float32).astype(jnp.bfloat16)
    slot_count = tokens.shape[0] // PATCH
    blocks = packed.reshape(slot_count, PATCH, 3 * channels)

    def one_patch(element):
        patch_rows, length = element
        key_mask = jnp.arange(PATCH) < length
        return attend(patch_rows[:, :channels], patch_rows[:, channels:2 * channels], patch_rows[:, 2 * channels:], channels // HD, key_mask)
    return lax.map(one_patch, (blocks, patch_count)).reshape(tokens.shape[0], channels)

def parent_table(offset):
    return (offset[:, None] == jnp.arange(Q_DEV + SPILL, dtype=jnp.int32)[None, :]).astype(jnp.float32)

def pool_counts(live_mask, offset):
    return jnp.dot(live_mask[None, :], parent_table(offset), precision=lax.Precision.HIGHEST)[0]

def pool_forward(out_weight, pooling, tokens, mixed_rows, live_mask, offset):
    fine_out = (tokens.astype(jnp.float32) + jnp.dot(mixed_rows, out_weight.astype(jnp.bfloat16), preferred_element_type=jnp.float32)).astype(jnp.bfloat16)
    projected = jnp.dot(fine_out, pooling.astype(jnp.bfloat16), preferred_element_type=jnp.float32) * live_mask[:, None]
    summed = jnp.dot(parent_table(offset).T, projected, precision=lax.Precision.HIGHEST)
    return (summed[:Q_DEV], summed[Q_DEV:])

def coarse_forward(own_sum, arrived, qkv_weight, divisor):
    summed = own_sum + jnp.pad(arrived, ((0, Q_DEV - SPILL), (0, 0)))
    coarse_in = jax.nn.gelu(summed / divisor[:, None]).astype(jnp.bfloat16)
    normed = normalize(coarse_in.astype(jnp.float32)).astype(jnp.bfloat16)
    packed = jnp.dot(normed, qkv_weight.astype(jnp.bfloat16), preferred_element_type=jnp.float32).astype(jnp.bfloat16)
    channels = coarse_in.shape[1]
    return (coarse_in, packed[:, :channels], packed[:, channels:2 * channels], packed[:, 2 * channels:])

def coarse_attention(coarse_in, queries, key_rows, value_rows, far_keys, far_values, out_weight):
    all_keys = jnp.concatenate([key_rows, far_keys], 0).astype(jnp.bfloat16)
    all_values = jnp.concatenate([value_rows, far_values], 0).astype(jnp.bfloat16)
    mixed_rows = attend(queries, all_keys, all_values, queries.shape[1] // HD, None)
    return (coarse_in.astype(jnp.float32) + jnp.dot(mixed_rows, out_weight.astype(jnp.bfloat16), preferred_element_type=jnp.float32)).astype(jnp.bfloat16)

def reference(fine_points, parent, patch_count, qkv_fine, out_fine, pool_weight, qkv_coarse, out_coarse, cotangent):
    devices = N_REP * N_PTS
    slot_count = P_DEV // PATCH
    channels = fine_points.shape[1]
    coarse_width = qkv_coarse.shape[0]
    tokens_all = fine_points.reshape(devices, P_DEV, channels)
    offsets = (parent.reshape(devices, P_DEV) - (jnp.arange(devices, dtype=jnp.int32) * Q_DEV)[:, None]).astype(jnp.int32)
    counts_all = patch_count.reshape(devices, slot_count)
    out_fine_wide = out_fine.astype(jnp.float32)
    pool_wide = pool_weight.astype(jnp.float32)
    qkv_wide = qkv_coarse.astype(jnp.float32)
    out_coarse_wide = out_coarse.astype(jnp.float32)

    def first_pass(element):
        tokens, offset, length = element
        mixed_rows = fine_attention(tokens, qkv_fine, length)
        live_mask = (jnp.arange(PATCH)[None, :] < length[:, None]).reshape(P_DEV).astype(jnp.float32)
        live_total = pool_counts(live_mask, offset)
        own_sum, spill_sum = pool_forward(out_fine_wide, pool_wide, tokens, mixed_rows, live_mask, offset)
        return (mixed_rows, live_mask, own_sum, spill_sum, live_total)
    mixed_all, live_all, own_all, spill_all, live_totals = lax.map(first_pass, (tokens_all, offsets, counts_all))

    def shift_down(stacked):
        grouped = stacked.reshape((N_REP, N_PTS) + stacked.shape[1:])
        moved = jnp.concatenate([jnp.zeros_like(grouped[:, :1]), grouped[:, :-1]], 1)
        return moved.reshape(stacked.shape)

    def shift_up(stacked):
        grouped = stacked.reshape((N_REP, N_PTS) + stacked.shape[1:])
        moved = jnp.concatenate([grouped[:, 1:], jnp.zeros_like(grouped[:, :1])], 1)
        return moved.reshape(stacked.shape)

    def swap_pairs(stacked):
        grouped = stacked.reshape((devices // 2, 2) + stacked.shape[1:])
        return grouped[:, ::-1].reshape(stacked.shape)
    arrived_all = shift_down(spill_all)
    arrived_counts = shift_down(live_totals[:, Q_DEV:])
    divisors = jnp.maximum(live_totals[:, :Q_DEV] + jnp.pad(arrived_counts, ((0, 0), (0, Q_DEV - SPILL))), 1.0)

    def second_pass(element):
        own_sum, arrived, divisor = element
        return coarse_forward(own_sum, arrived, qkv_wide, divisor)
    coarse_in_all, query_all, key_all, value_all = lax.map(second_pass, (own_all, arrived_all, divisors))
    far_key_all = swap_pairs(key_all)
    far_value_all = swap_pairs(value_all)

    def third_pass(element):
        coarse_in, queries, key_rows, value_rows, far_keys, far_values, grad_out = element
        coarse_rows, backward = jax.vjp(coarse_attention, coarse_in, queries, key_rows.astype(jnp.float32), value_rows.astype(jnp.float32), far_keys.astype(jnp.float32), far_values.astype(jnp.float32), out_coarse_wide)
        return (coarse_rows,) + tuple(backward(grad_out))
    grad_rows = cotangent.reshape(devices, Q_DEV, coarse_width)
    results = lax.map(third_pass, (coarse_in_all, query_all, key_all, value_all, far_key_all, far_value_all, grad_rows))
    coarse_all, grad_in, grad_query, grad_key, grad_value, grad_far_key, grad_far_value, grad_out_coarse = results
    back_key = swap_pairs(grad_far_key.astype(jnp.bfloat16))
    back_value = swap_pairs(grad_far_value.astype(jnp.bfloat16))
    total_key = (grad_key + back_key.astype(jnp.float32)).astype(jnp.bfloat16)
    total_value = (grad_value + back_value.astype(jnp.float32)).astype(jnp.bfloat16)

    def fourth_pass(element):
        own_sum, arrived, divisor, grad_coarse_in, grad_queries, grad_keys, grad_values = element

        def local_part(own_part, arrived_part, qkv_part):
            return coarse_forward(own_part, arrived_part, qkv_part, divisor)
        unused, backward = jax.vjp(local_part, own_sum, arrived, qkv_wide)
        return backward((grad_coarse_in, grad_queries, grad_keys, grad_values))
    grad_own, grad_arrived, grad_qkv_coarse = lax.map(fourth_pass, (own_all, arrived_all, divisors, grad_in, grad_query, total_key, total_value))
    grad_spill = shift_up(grad_arrived)

    def fifth_pass(element):
        tokens, mixed_rows, live_mask, offset, grad_own_rows, grad_spill_rows = element

        def local_part(out_weight, pooling):
            return pool_forward(out_weight, pooling, tokens, mixed_rows, live_mask, offset)
        unused, backward = jax.vjp(local_part, out_fine_wide, pool_wide)
        return backward((grad_own_rows, grad_spill_rows))
    grad_out_fine, grad_pool = lax.map(fifth_pass, (tokens_all, mixed_all, live_all, offsets, grad_own, grad_spill))

    def reduce_all(stacked):
        grouped = stacked.astype(jnp.float32).reshape((N_REP, N_PTS) + stacked.shape[1:])
        group_sum = lax.optimization_barrier(lax.optimization_barrier(jnp.sum(grouped, 1)).astype(jnp.bfloat16)).astype(jnp.float32)
        return lax.optimization_barrier(jnp.sum(group_sum, 0)).astype(jnp.bfloat16)
    return (coarse_all.reshape(devices * Q_DEV, coarse_width), reduce_all(grad_out_fine), reduce_all(grad_pool), reduce_all(grad_qkv_coarse), reduce_all(grad_out_coarse))
```

```python
import jax
import jax.numpy as jnp
from jax import lax
from jax.experimental import pallas as pl
from jax.experimental.pallas import tpu as pltpu
from jax.sharding import PartitionSpec as P

F32 = jnp.float32
BF = jnp.bfloat16
EPS = 1e-6
LOG2E = 1.4426950408889634
LN2 = 0.6931471805599453
SAFE = 80.0
MESH = pl.DeviceIdType.MESH
VM = pl.BlockSpec(memory_space=pltpu.VMEM)
SM = pl.BlockSpec(memory_space=pltpu.SMEM)

NN = (((1,), (0,)), ((), ()))
NT = (((1,), (1,)), ((), ()))
TN = (((0,), (0,)), ((), ()))
TT = (((0,), (1,)), ((), ()))


def mm(a, b, dims=NN):
    return lax.dot_general(a, b, dims, preferred_element_type=F32)


def normalize(values):
    return values * lax.rsqrt(jnp.mean(values * values, axis=-1, keepdims=True) + EPS)


def split_dot(a, b):
    high = a.astype(BF)
    low = (a - high.astype(F32)).astype(BF)
    return mm(high, b) + mm(low, b)


def head_rows(rows, width):
    return lax.broadcasted_iota(jnp.int32, (rows, width), 0) // 16


def score_bound(qt, k):
    channels = qt.shape[0]
    heads = (
        lax.broadcasted_iota(jnp.int32, (channels, 128), 0) // 16
        == lax.broadcasted_iota(jnp.int32, (channels, 128), 1)
    ).astype(BF)
    kf = k.astype(F32)
    k2 = mm((kf * kf).astype(BF), heads)
    q = qt.astype(F32)
    q2 = (q * q).reshape(channels // 16, 16, qt.shape[1]).sum(axis=1)
    return jnp.max(q2) * jnp.max(k2)


def fine_kernel(cnt_ref, off_ref, x_ref, w_ref, ow_ref, ab_ref, k_ref, qt_ref, va_ref, mt_ref):
    count = cnt_ref[0]
    x = x_ref[...]
    n = normalize(x.astype(F32)).astype(BF)
    k_ref[...] = mm(n, w_ref[:, 256:512]).astype(BF)
    qt_ref[...] = (mm(w_ref[:, :256], n, TT) * (0.25 * LOG2E)).astype(BF)
    vt = mm(w_ref[:, 512:], n, TT).astype(BF)
    live = lax.broadcasted_iota(jnp.int32, (1, 1024), 1) < count
    ones = jnp.where(jnp.broadcast_to(live, (16, 1024)), 1.0, 0.0).astype(BF)
    for h in range(16):
        rows = vt[h * 16 : h * 16 + 16, :].astype(F32)
        va_ref[h, 0:16, :] = jnp.where(live, rows, 0.0).astype(BF)
        va_ref[h, 16:32, :] = ones
    bound = score_bound(qt_ref[...], k_ref[...])
    quick = bound < SAFE * SAFE

    def attend(shift):
        def head(h, carry):
            half = pl.multiple_of((h // 8) * 128, 128)
            keys = k_ref[:, pl.ds(half, 128)]
            chosen = head_rows(128, 256) == h % 8
            row = pl.multiple_of(h * 16, 16)
            for t in range(4):
                cols = slice(t * 256, t * 256 + 256)
                part = qt_ref[pl.ds(half, 128), cols]
                qm = jnp.where(chosen, part, jnp.zeros_like(part))
                s = mm(keys, qm)
                if shift:
                    alive = lax.broadcasted_iota(jnp.int32, (1024, 256), 0) < count
                    s = jnp.where(alive, s, -1e30)
                    s = s - jnp.max(s, axis=0, keepdims=True)
                p = jnp.exp2(s).astype(BF)
                o = mm(va_ref[h], p)
                mt_ref[pl.ds(row, 16), cols] = (o[:16] / o[16:]).astype(BF)
            return carry

        lax.fori_loop(0, 16, head, 0)

    @pl.when(quick)
    def _():
        attend(False)

    @pl.when(jnp.logical_not(quick))
    def _():
        attend(True)

    table = jnp.where(
        (lax.broadcasted_iota(jnp.int32, (288, 1024), 0) == off_ref[...]) & live, 1.0, 0.0
    )
    total = jnp.sum(table, axis=1, keepdims=True)
    table = table.astype(BF)
    b = mm(table, mt_ref[...], NT)
    ab_ref[:, :256] = mm(table, x) + split_dot(b, ow_ref[...])
    ab_ref[:, 256:512] = b
    ab_ref[:, 512:] = jnp.broadcast_to(total, (288, 128))


def fine_call(count, offset, x, w, ow):
    return pl.pallas_call(
        fine_kernel,
        out_shape=jax.ShapeDtypeStruct((288, 640), F32),
        in_specs=[SM, VM, VM, VM, VM],
        out_specs=VM,
        scratch_shapes=[
            pltpu.VMEM((1024, 256), BF),
            pltpu.VMEM((256, 1024), BF),
            pltpu.VMEM((16, 32, 1024), BF),
            pltpu.VMEM((256, 1024), BF),
        ],
        compiler_params=pltpu.CompilerParams(vmem_limit_bytes=56 * 1024 * 1024),
        name="fine",
    )(count, offset, x, w, ow)


def pooled(ab_ref, arr_ref, first, last):
    top = ab_ref[:32, first:last] + arr_ref[:, first:last]
    return jnp.concatenate([top, ab_ref[32:256, first:last]], axis=0)


def pooled_mean(ab_ref, arr_ref, pw_ref):
    a = pooled(ab_ref, arr_ref, 0, 256)
    count = jnp.maximum(pooled(ab_ref, arr_ref, 512, 640)[:, :1], 1.0)
    return split_dot(a, pw_ref[...]) / count, count


GA = 0.7978845608028654
GB = 0.044715


def coarse_in_kernel(ab_ref, arr_ref, pw_ref, c_ref):
    u, _ = pooled_mean(ab_ref, arr_ref, pw_ref)
    c_ref[...] = (0.5 * u * (1.0 + jnp.tanh(GA * (u + GB * u * u * u)))).astype(BF)


def coarse_kernel(
    core_ref, c_ref, cf_ref, ct_ref, ctf_ref, w_ref, ow_ref,
    dn_ref, mix_ref, g_ref,
    n_ref, cot_ref, k_ref, v_ref, kt_ref, qt_ref, va_ref, dot_ref, ot_ref, dp_ref,
):
    core = core_ref[0]
    lo = pl.multiple_of(core * 256, 256)
    n_ref[:256] = normalize(c_ref[...].astype(F32)).astype(BF)
    n_ref[256:] = normalize(cf_ref[...].astype(F32)).astype(BF)
    cot_ref[:256] = ct_ref[...]
    cot_ref[256:] = ctf_ref[...]
    n = n_ref[...]
    wq = w_ref[:, pl.ds(lo, 256)]
    wk = w_ref[:, pl.ds(512 + lo, 256)]
    wv = w_ref[:, pl.ds(1024 + lo, 256)]
    qt_ref[...] = (mm(wq, n, TT) * (0.25 * LOG2E)).astype(BF)
    k_ref[...] = mm(n, wk).astype(BF)
    v_ref[...] = mm(n, wv).astype(BF)
    kt_ref[...] = mm(wk, n, TT).astype(BF)
    vt = mm(wv, n, TT).astype(BF)
    for h in range(16):
        va_ref[h, :16, :] = vt[h * 16 : h * 16 + 16, :]
        va_ref[h, 16:, :] = jnp.ones((16, 512), BF)
    dot_ref[...] = mm(ow_ref[pl.ds(lo, 256), :], cot_ref[...], NT)
    quick = score_bound(qt_ref[...], k_ref[...]) < SAFE * SAFE

    def attend(shift):
        def head(h, carry):
            half = pl.multiple_of((h // 8) * 128, 128)
            chosen = head_rows(128, 512) == h % 8
            row = pl.multiple_of(h * 16, 16)
            part = qt_ref[pl.ds(half, 128), :]
            qm = jnp.where(chosen, part, jnp.zeros_like(part))
            s = mm(k_ref[:, pl.ds(half, 128)], qm)
            if shift:
                s = s - jnp.max(s, axis=0, keepdims=True)
            p = jnp.exp2(s)
            pb = p.astype(BF)
            o = mm(va_ref[h], pb)
            inverse = 1.0 / o[16:]
            on = o[:16] * inverse
            ot_ref[pl.ds(row, 16), :] = on.astype(BF)
            do = dot_ref[pl.ds(row, 16), :] * inverse
            dob = do.astype(BF)
            delta = jnp.sum(dob.astype(F32) * on, axis=0, keepdims=True)
            tiled = jnp.concatenate([dob] * 8, axis=0)
            dom = jnp.where(chosen, tiled, jnp.zeros_like(tiled))
            dpt = mm(v_ref[:, pl.ds(half, 128)], dom)
            ds = (p * (dpt - delta)).astype(BF)
            dp_ref[pl.ds(row, 16), :] = (mm(kt_ref[pl.ds(row, 16), :], ds) * 0.25).astype(BF)
            dk = mm(qt_ref[pl.ds(row, 16), :], ds, NT) * LN2
            dp_ref[pl.ds(256 + row, 16), :] = dk.astype(BF)
            dp_ref[pl.ds(512 + row, 16), :] = mm(dob, pb, NT).astype(BF)
            return carry

        lax.fori_loop(0, 16, head, 0)

    @pl.when(quick)
    def _():
        attend(False)

    @pl.when(jnp.logical_not(quick))
    def _():
        attend(True)

    mix_ref[...] = jnp.transpose(ot_ref[...])
    dnt = (
        mm(wq, dp_ref[:256, :]) + mm(wk, dp_ref[256:512, :]) + mm(wv, dp_ref[512:, :])
    ).astype(BF)
    dn_ref[...] = jnp.transpose(dnt)
    nt = jnp.transpose(n_ref[...])
    for j in range(6):
        block = mm(nt, dp_ref[j * 128 : j * 128 + 128, :], NT).astype(BF)
        g_ref[j * 32 : j * 32 + 32] = block.reshape(32, 16, 128)
    for j in range(4):
        block = mm(ot_ref[...], cot_ref[:, j * 128 : j * 128 + 128]).astype(BF)
        g_ref[192 + j * 16 : 208 + j * 16] = block.reshape(16, 16, 128)


def coarse_call(core, c, cf, ct, ctf, w, ow):
    return pl.pallas_call(
        coarse_kernel,
        out_shape=(
            jax.ShapeDtypeStruct((512, 512), BF),
            jax.ShapeDtypeStruct((512, 256), BF),
            jax.ShapeDtypeStruct((256, 16, 128), BF),
        ),
        in_specs=[SM, VM, VM, VM, VM, VM, VM],
        out_specs=(VM, VM, VM),
        scratch_shapes=[
            pltpu.VMEM((512, 512), BF),
            pltpu.VMEM((512, 512), BF),
            pltpu.VMEM((512, 256), BF),
            pltpu.VMEM((512, 256), BF),
            pltpu.VMEM((256, 512), BF),
            pltpu.VMEM((256, 512), BF),
            pltpu.VMEM((16, 32, 512), BF),
            pltpu.VMEM((256, 512), F32),
            pltpu.VMEM((256, 512), BF),
            pltpu.VMEM((768, 512), BF),
        ],
        compiler_params=pltpu.CompilerParams(vmem_limit_bytes=56 * 1024 * 1024),
        name="coarse",
    )(core, c, cf, ct, ctf, w, ow)


def finish_kernel(
    core_ref, ab_ref, arr_ref, pw_ref, c_ref, ct_ref, dn_ref, dnf_ref, mix_ref, mixf_ref,
    ow_ref, out_ref, g_ref,
):
    core = core_ref[0]
    lo = pl.multiple_of(core * 256, 256)
    hi = pl.multiple_of(256 - core * 256, 256)
    c = c_ref[...].astype(F32)
    mixed = mm(mix_ref[:256], ow_ref[pl.ds(lo, 256), :]) + mm(mixf_ref[...], ow_ref[pl.ds(hi, 256), :])
    out_ref[...] = (c + mixed).astype(BF)
    dn = dn_ref[:256].astype(F32) + dnf_ref[...].astype(F32)
    r = lax.rsqrt(jnp.mean(c * c, axis=-1, keepdims=True) + EPS)
    inner = jnp.mean(dn * c, axis=-1, keepdims=True)
    dc = r * dn - c * (r * r * r * inner) + ct_ref[...].astype(F32)
    u, count = pooled_mean(ab_ref, arr_ref, pw_ref)
    th = jnp.tanh(GA * (u + GB * u * u * u))
    slope = 0.5 * (1.0 + th) + 0.5 * u * (1.0 - th * th) * (GA * (1.0 + 3.0 * GB * u * u))
    gs = (slope * dc / count).astype(BF)
    at = jnp.transpose(pooled(ab_ref, arr_ref, 0, 256)).astype(BF)
    bt = jnp.transpose(pooled(ab_ref, arr_ref, 256, 512)).astype(BF)
    gw = mm(gs, pw_ref[...], NT).astype(BF)
    for half in range(2):
        rows = slice(half * 128, half * 128 + 128)
        for j in range(4):
            block = mm(at[rows], gs[:, j * 128 : j * 128 + 128]).astype(BF)
            g_ref[half, j * 8 : j * 8 + 8] = block.reshape(8, 16, 128)
        for j in range(2):
            block = mm(bt[rows], gw[:, j * 128 : j * 128 + 128]).astype(BF)
            g_ref[half, 32 + j * 8 : 40 + j * 8] = block.reshape(8, 16, 128)


def reduce_kernel(
    big_ref, small_ref, gof_ref, gp_ref, gq_ref, goc_ref,
    g, full, sm, ra, rb, ha, hb, ra2, rb2, z, rz, zf, fa, fb, send, recv,
):
    rep = lax.axis_index("rep")
    pts = lax.axis_index("pts")
    x = rep % 4
    zlo = rep // 4
    y = pts // 8
    zhi = (pts // 2) % 4
    core = pts % 2
    zi = zhi * 2 + zlo

    def xpeer(d):
        return (zlo * 4 + (x + d) % 4, pts)

    def ypeer(d):
        return (rep, ((y + d) % 4) * 8 + zhi * 2 + core)

    def zpeer(d):
        other = (zi + d) % 8
        return ((other % 2) * 4 + x, y * 8 + (other // 2) * 2 + core)

    partner = (rep, pts + 1 - 2 * core)
    barrier = pltpu.get_barrier_semaphore()
    peers = [partner]
    peers += [xpeer(d) for d in (1, 2, 3)] + [ypeer(d) for d in (1, 2, 3)]
    peers += [zpeer(d) for d in range(1, 8)]
    for peer in peers:
        pl.semaphore_signal(barrier, inc=1, device_id=peer, device_id_type=MESH)
    pl.semaphore_wait(barrier, len(peers))

    counter = [0]

    def push(src, dst, peer):
        i = counter[0]
        counter[0] += 1
        copy = pltpu.make_async_remote_copy(
            src_ref=src, dst_ref=dst, send_sem=send.at[i], recv_sem=recv.at[i],
            device_id=peer, device_id_type=MESH,
        )
        copy.start()
        return copy

    swap = push(small_ref.at[1 - core], sm, partner)
    g[:256] = big_ref[...]
    g[304:] = jnp.zeros((16, 16, 128), BF)
    first = []
    for d in (1, 2, 3):
        to = (x + d) % 4
        first.append(push(g.at[pl.ds(to * 40, 40)], ra.at[d - 1], xpeer(d)))
    swap.wait()
    g[256:304] = (small_ref[core].astype(F32) + sm[...].astype(F32)).astype(BF)
    for d in (1, 2, 3):
        to = (y + d) % 4
        first.append(push(g.at[pl.ds(160 + to * 40, 40)], rb.at[d - 1], ypeer(d)))
    for copy in first:
        copy.wait()

    def add(own, slots, n):
        total = own.astype(F32)
        for d in range(n):
            total = total + slots[d].astype(F32)
        return total.astype(BF)

    ha[...] = add(g[pl.ds(x * 40, 40)], ra, 3)
    hb[...] = add(g[pl.ds(160 + y * 40, 40)], rb, 3)
    second = []
    for d in (1, 2, 3):
        second.append(push(ha.at[pl.ds(((y + d) % 4) * 10, 10)], ra2.at[d - 1], ypeer(d)))
        second.append(push(hb.at[pl.ds(((x + d) % 4) * 10, 10)], rb2.at[d - 1], xpeer(d)))
    for copy in second:
        copy.wait()
    z[:10] = add(ha[pl.ds(y * 10, 10)], ra2, 3)
    z[10:20] = add(hb[pl.ds(x * 10, 10)], rb2, 3)
    z[20:] = jnp.zeros((4, 16, 128), BF)
    third = []
    for d in range(1, 8):
        third.append(push(z.at[pl.ds(((zi + d) % 8) * 3, 3)], rz.at[d - 1], zpeer(d)))
    for copy in third:
        copy.wait()
    mine = pl.ds(zi * 3, 3)
    zf[mine] = add(z[mine], rz, 7)
    back = [push(zf.at[mine], zf.at[mine], zpeer(d)) for d in range(1, 8)]
    for copy in back:
        copy.wait()
    at, bt = pl.ds(y * 10, 10), pl.ds(x * 10, 10)
    fa[at] = zf[:10]
    fb[bt] = zf[10:20]
    back = []
    for d in (1, 2, 3):
        back.append(push(fa.at[at], fa.at[at], ypeer(d)))
        back.append(push(fb.at[bt], fb.at[bt], xpeer(d)))
    for copy in back:
        copy.wait()
    at, bt = pl.ds(x * 40, 40), pl.ds(160 + y * 40, 40)
    full[core, at] = fa[...]
    full[core, bt] = fb[...]
    back = []
    for d in (1, 2, 3):
        back.append(push(full.at[core, at], full.at[core, at], xpeer(d)))
        back.append(push(full.at[core, bt], full.at[core, bt], ypeer(d)))
    for copy in back:
        copy.wait()
    push(full.at[core], full.at[core], partner).wait()
    for c in range(2):
        for j in range(6):
            column = (j // 2) * 512 + c * 256 + (j % 2) * 128
            gq_ref[:, column : column + 128] = full[c, j * 32 : j * 32 + 32].reshape(512, 128)
        for j in range(4):
            rows = slice(c * 256, c * 256 + 256)
            tile = full[c, 192 + j * 16 : 208 + j * 16].reshape(256, 128)
            goc_ref[rows, j * 128 : j * 128 + 128] = tile
        rows = slice(c * 128, c * 128 + 128)
        for j in range(4):
            tile = full[c, 256 + j * 8 : 264 + j * 8].reshape(128, 128)
            gp_ref[rows, j * 128 : j * 128 + 128] = tile
        for j in range(2):
            tile = full[c, 288 + j * 8 : 296 + j * 8].reshape(128, 128)
            gof_ref[rows, j * 128 : j * 128 + 128] = tile


def reduce_call(big, small):
    def tiles(*n):
        return pltpu.VMEM((*n, 16, 128), BF)

    return pl.pallas_call(
        reduce_kernel,
        out_shape=(
            jax.ShapeDtypeStruct((256, 256), BF),
            jax.ShapeDtypeStruct((256, 512), BF),
            jax.ShapeDtypeStruct((512, 1536), BF),
            jax.ShapeDtypeStruct((512, 512), BF),
        ),
        in_specs=[VM, VM],
        out_specs=(VM, VM, VM, VM),
        scratch_shapes=[
            tiles(320), tiles(2, 320), tiles(48), tiles(3, 40), tiles(3, 40), tiles(40), tiles(40),
            tiles(3, 10), tiles(3, 10), tiles(24), tiles(7, 3), tiles(24), tiles(40), tiles(40),
            pltpu.SemaphoreType.DMA((40,)),
            pltpu.SemaphoreType.DMA((40,)),
        ],
        compiler_params=pltpu.CompilerParams(
            collective_id=0, has_side_effects=True, vmem_limit_bytes=40 * 1024 * 1024
        ),
        name="reduce",
    )(big, small)


def local(
    fine_points, parent, patch_count, qkv_fine, out_fine, pool_weight, qkv_coarse, out_coarse,
    cotangent,
):
    pts = lax.axis_index("pts")
    position = lax.axis_index("rep") * lax.axis_size("pts") + pts
    core = (pts % 2).reshape(1)
    swap = [(i, i ^ 1) for i in range(32)]
    far_cot = lax.ppermute(cotangent, "pts", swap)
    offset = (parent - position * 256).reshape(1, 1024)
    ab = fine_call(patch_count, offset, fine_points, qkv_fine, out_fine)
    arrived = lax.ppermute(ab[256:], "pts", [(i, i + 1) for i in range(31)])
    coarse_in = pl.pallas_call(
        coarse_in_kernel,
        out_shape=jax.ShapeDtypeStruct((256, 512), BF),
        in_specs=[VM, VM, VM],
        out_specs=VM,
        name="coarse_in",
    )(ab, arrived, pool_weight)
    far_in = lax.ppermute(coarse_in, "pts", swap)
    dn, mixed, big = coarse_call(core, coarse_in, far_in, cotangent, far_cot, qkv_coarse, out_coarse)
    far_dn, far_mixed = lax.ppermute((dn[256:], mixed[256:]), "pts", swap)
    coarse_out, small = pl.pallas_call(
        finish_kernel,
        out_shape=(
            jax.ShapeDtypeStruct((256, 512), BF),
            jax.ShapeDtypeStruct((2, 48, 16, 128), BF),
        ),
        in_specs=[SM] + [VM] * 10,
        out_specs=(VM, VM),
        name="finish",
    )(core, ab, arrived, pool_weight, coarse_in, cotangent, dn, far_dn, mixed, far_mixed, out_coarse)
    grads = reduce_call(big, small)
    return (coarse_out, *grads)


def solution(mesh):
    rows = P(("rep", "pts"), None)
    flat = P(("rep", "pts"))
    return jax.shard_map(
        local,
        mesh=mesh,
        in_specs=(rows, flat, flat, P(), P(), P(), P(), P(), rows),
        out_specs=(rows, P(), P(), P(), P()),
        check_vma=False,
    )
```

```python
import jax
import jax.numpy as jnp
from jax import lax
from jax.experimental import pallas as pl
from jax.experimental.pallas import tpu as pltpu
from jax.sharding import PartitionSpec as P

F32 = jnp.float32
BF = jnp.bfloat16
EPS = 1e-6
LOG2E = 1.4426950408889634
LN2 = 0.6931471805599453
SAFE = 80.0
MESH = pl.DeviceIdType.MESH
VM = pl.BlockSpec(memory_space=pltpu.VMEM)
SM = pl.BlockSpec(memory_space=pltpu.SMEM)

NN = (((1,), (0,)), ((), ()))
NT = (((1,), (1,)), ((), ()))
TN = (((0,), (0,)), ((), ()))
TT = (((0,), (1,)), ((), ()))


def mm(a, b, dims=NN):
    return lax.dot_general(a, b, dims, preferred_element_type=F32)


def normalize(values):
    return values * lax.rsqrt(jnp.mean(values * values, axis=-1, keepdims=True) + EPS)


def split_dot(a, b):
    high = a.astype(BF)
    low = (a - high.astype(F32)).astype(BF)
    return mm(high, b) + mm(low, b)


def head_rows(rows, width):
    return lax.broadcasted_iota(jnp.int32, (rows, width), 0) // 16


def score_bound(qt, k):
    channels = qt.shape[0]
    heads = (
        lax.broadcasted_iota(jnp.int32, (channels, 128), 0) // 16
        == lax.broadcasted_iota(jnp.int32, (channels, 128), 1)
    ).astype(BF)
    kf = k.astype(F32)
    k2 = mm((kf * kf).astype(BF), heads)
    q = qt.astype(F32)
    q2 = (q * q).reshape(channels // 16, 16, qt.shape[1]).sum(axis=1)
    return jnp.max(q2) * jnp.max(k2)


def fine_kernel(cnt_ref, off_ref, x_ref, w_ref, ow_ref, ab_ref, k_ref, qt_ref, va_ref, mt_ref):
    count = cnt_ref[0]
    x = x_ref[...]
    n = normalize(x.astype(F32)).astype(BF)
    k_ref[...] = mm(n, w_ref[:, 256:512]).astype(BF)
    qt_ref[...] = (mm(w_ref[:, :256], n, TT) * (0.25 * LOG2E)).astype(BF)
    vt = mm(w_ref[:, 512:], n, TT).astype(BF)
    live = lax.broadcasted_iota(jnp.int32, (1, 1024), 1) < count
    ones = jnp.where(jnp.broadcast_to(live, (16, 1024)), 1.0, 0.0).astype(BF)
    for h in range(16):
        rows = vt[h * 16 : h * 16 + 16, :].astype(F32)
        va_ref[h, 0:16, :] = jnp.where(live, rows, 0.0).astype(BF)
        va_ref[h, 16:32, :] = ones
    bound = score_bound(qt_ref[...], k_ref[...])
    quick = bound < SAFE * SAFE

    def safe_head(h, carry):
        half = pl.multiple_of((h // 8) * 128, 128)
        row = pl.multiple_of(h * 16, 16)
        chosen = head_rows(128, 256) == h % 8
        alive = lax.broadcasted_iota(jnp.int32, (1024, 256), 0) < count
        for t in range(4):
            cols = slice(t * 256, t * 256 + 256)
            part = qt_ref[pl.ds(half, 128), cols]
            s = mm(k_ref[:, pl.ds(half, 128)], jnp.where(chosen, part, jnp.zeros_like(part)))
            s = jnp.where(alive, s, -1e30)
            s = s - jnp.max(s, axis=0, keepdims=True)
            o = mm(va_ref[h], jnp.exp2(s).astype(BF))
            mt_ref[pl.ds(row, 16), cols] = (o[:16] / o[16:]).astype(BF)
        return carry

    def quick_head(h, carry):
        half = pl.multiple_of((h // 8) * 128, 128)
        row = pl.multiple_of(h * 16, 16)
        ck, cq = 1024, 256
        units = [(t, c) for t in range(1024 // cq) for c in range(1024 // ck)]
        chosen = head_rows(128, cq) == h % 8
        scores, weights, sums, queries = {}, {}, {}, {}
        for i in range(len(units) + 2):
            if i < len(units):
                t, c = units[i]
                if c == 0:
                    part = qt_ref[pl.ds(half, 128), t * cq : t * cq + cq]
                    queries[t] = jnp.where(chosen, part, jnp.zeros_like(part))
                scores[i] = mm(k_ref[c * ck : c * ck + ck, pl.ds(half, 128)], queries[t])
            if 1 <= i <= len(units):
                weights[i - 1] = jnp.exp2(scores.pop(i - 1)).astype(BF)
            if i >= 2:
                t, c = units[i - 2]
                o = mm(va_ref[h, :, c * ck : c * ck + ck], weights.pop(i - 2))
                sums[t] = o if c == 0 else sums[t] + o
                if c == 1024 // ck - 1:
                    o = sums.pop(t)
                    mt_ref[pl.ds(row, 16), t * cq : t * cq + cq] = (o[:16] / o[16:]).astype(BF)
        return carry

    @pl.when(quick)
    def _():
        lax.fori_loop(0, 16, quick_head, 0, unroll=4)

    @pl.when(jnp.logical_not(quick))
    def _():
        lax.fori_loop(0, 16, safe_head, 0)

    table = jnp.where(
        (lax.broadcasted_iota(jnp.int32, (288, 1024), 0) == off_ref[...]) & live, 1.0, 0.0
    )
    total = jnp.sum(table, axis=1, keepdims=True)
    table = table.astype(BF)
    b = mm(table, mt_ref[...], NT)
    ab_ref[:, :256] = mm(table, x) + split_dot(b, ow_ref[...])
    ab_ref[:, 256:512] = b
    ab_ref[:, 512:] = jnp.broadcast_to(total, (288, 128))


def fine_call(count, offset, x, w, ow):
    return pl.pallas_call(
        fine_kernel,
        out_shape=jax.ShapeDtypeStruct((288, 640), F32),
        in_specs=[SM, VM, VM, VM, VM],
        out_specs=VM,
        scratch_shapes=[
            pltpu.VMEM((1024, 256), BF),
            pltpu.VMEM((256, 1024), BF),
            pltpu.VMEM((16, 32, 1024), BF),
            pltpu.VMEM((256, 1024), BF),
        ],
        compiler_params=pltpu.CompilerParams(vmem_limit_bytes=56 * 1024 * 1024),
        name="fine",
    )(count, offset, x, w, ow)


def pooled(ab_ref, arr_ref, first, last):
    top = ab_ref[:32, first:last] + arr_ref[:, first:last]
    return jnp.concatenate([top, ab_ref[32:256, first:last]], axis=0)


def pooled_mean(ab_ref, arr_ref, pw_ref):
    a = pooled(ab_ref, arr_ref, 0, 256)
    count = jnp.maximum(pooled(ab_ref, arr_ref, 512, 640)[:, :1], 1.0)
    return split_dot(a, pw_ref[...]) / count, count


GA = 0.7978845608028654
GB = 0.044715


def coarse_in_kernel(ab_ref, arr_ref, pw_ref, c_ref):
    u, _ = pooled_mean(ab_ref, arr_ref, pw_ref)
    c_ref[...] = (0.5 * u * (1.0 + jnp.tanh(GA * (u + GB * u * u * u)))).astype(BF)


def coarse_kernel(
    core_ref, c_ref, cf_ref, ct_ref, ctf_ref, w_ref, ow_ref,
    dn_ref, mix_ref, g_ref,
    n_ref, cot_ref, k_ref, v_ref, kt_ref, qt_ref, va_ref, dot_ref, ot_ref, dp_ref,
    p_ref, pb_ref, ds_ref,
):
    core = core_ref[0]
    lo = pl.multiple_of(core * 256, 256)
    n_ref[:256] = normalize(c_ref[...].astype(F32)).astype(BF)
    n_ref[256:] = normalize(cf_ref[...].astype(F32)).astype(BF)
    cot_ref[:256] = ct_ref[...]
    cot_ref[256:] = ctf_ref[...]
    n = n_ref[...]
    wq = w_ref[:, pl.ds(lo, 256)]
    wk = w_ref[:, pl.ds(512 + lo, 256)]
    wv = w_ref[:, pl.ds(1024 + lo, 256)]
    qt_ref[...] = (mm(wq, n, TT) * (0.25 * LOG2E)).astype(BF)
    k_ref[...] = mm(n, wk).astype(BF)
    v_ref[...] = mm(n, wv).astype(BF)
    kt_ref[...] = mm(wk, n, TT).astype(BF)
    vt = mm(wv, n, TT).astype(BF)
    for h in range(16):
        va_ref[h, :16, :] = vt[h * 16 : h * 16 + 16, :]
        va_ref[h, 16:, :] = jnp.ones((16, 512), BF)
    dot_ref[...] = mm(ow_ref[pl.ds(lo, 256), :], cot_ref[...], NT)
    quick = score_bound(qt_ref[...], k_ref[...]) < SAFE * SAFE

    def stage_one(h, slot, shift):
        half = pl.multiple_of((h // 8) * 128, 128)
        row = pl.multiple_of(h * 16, 16)
        chosen = head_rows(128, 512) == h % 8
        part = qt_ref[pl.ds(half, 128), :]
        qm = jnp.where(chosen, part, jnp.zeros_like(part))
        s = mm(k_ref[:, pl.ds(half, 128)], qm)
        if shift:
            s = s - jnp.max(s, axis=0, keepdims=True)
        p = jnp.exp2(s)
        p_ref[slot] = p
        pb_ref[slot] = p.astype(BF)

    def stage_two(h, slot):
        half = pl.multiple_of((h // 8) * 128, 128)
        row = pl.multiple_of(h * 16, 16)
        chosen = head_rows(128, 512) == h % 8
        pb = pb_ref[slot]
        o = mm(va_ref[h], pb)
        inverse = 1.0 / o[16:]
        on = o[:16] * inverse
        ot_ref[pl.ds(row, 16), :] = on.astype(BF)
        do = dot_ref[pl.ds(row, 16), :] * inverse
        dob = do.astype(BF)
        delta = jnp.sum(dob.astype(F32) * on, axis=0, keepdims=True)
        tiled = jnp.concatenate([dob] * 8, axis=0)
        dom = jnp.where(chosen, tiled, jnp.zeros_like(tiled))
        dpt = mm(v_ref[:, pl.ds(half, 128)], dom)
        ds_ref[slot] = (p_ref[slot] * (dpt - delta)).astype(BF)
        dp_ref[pl.ds(512 + row, 16), :] = mm(dob, pb, NT).astype(BF)

    def stage_three(h, slot):
        row = pl.multiple_of(h * 16, 16)
        ds = ds_ref[slot]
        dp_ref[pl.ds(row, 16), :] = (mm(kt_ref[pl.ds(row, 16), :], ds) * 0.25).astype(BF)
        dk = mm(qt_ref[pl.ds(row, 16), :], ds, NT) * LN2
        dp_ref[pl.ds(256 + row, 16), :] = dk.astype(BF)

    def attend(shift):
        stage_one(0, 0, shift)
        stage_one(1, 1, shift)
        stage_two(0, 0)

        def step(j, carry):
            for e in (0, 1):
                h = 2 * j + e
                stage_two(h + 1, 1 - e)
                stage_three(h, e)
                stage_one(h + 2, e, shift)
            return carry

        lax.fori_loop(0, 7, step, 0)
        stage_two(15, 1)
        stage_three(14, 0)
        stage_three(15, 1)

    @pl.when(quick)
    def _():
        attend(False)

    @pl.when(jnp.logical_not(quick))
    def _():
        attend(True)

    mix_ref[...] = jnp.transpose(ot_ref[...])
    dnt = (
        mm(wq, dp_ref[:256, :]) + mm(wk, dp_ref[256:512, :]) + mm(wv, dp_ref[512:, :])
    ).astype(BF)
    dn_ref[...] = jnp.transpose(dnt)
    nt = jnp.transpose(n_ref[...])
    for j in range(6):
        block = mm(nt, dp_ref[j * 128 : j * 128 + 128, :], NT).astype(BF)
        g_ref[j * 32 : j * 32 + 32] = block.reshape(32, 16, 128)
    for j in range(4):
        block = mm(ot_ref[...], cot_ref[:, j * 128 : j * 128 + 128]).astype(BF)
        g_ref[192 + j * 16 : 208 + j * 16] = block.reshape(16, 16, 128)


def coarse_call(core, c, cf, ct, ctf, w, ow):
    return pl.pallas_call(
        coarse_kernel,
        out_shape=(
            jax.ShapeDtypeStruct((512, 512), BF),
            jax.ShapeDtypeStruct((512, 256), BF),
            jax.ShapeDtypeStruct((256, 16, 128), BF),
        ),
        in_specs=[SM, VM, VM, VM, VM, VM, VM],
        out_specs=(VM, VM, VM),
        scratch_shapes=[
            pltpu.VMEM((512, 512), BF),
            pltpu.VMEM((512, 512), BF),
            pltpu.VMEM((512, 256), BF),
            pltpu.VMEM((512, 256), BF),
            pltpu.VMEM((256, 512), BF),
            pltpu.VMEM((256, 512), BF),
            pltpu.VMEM((16, 32, 512), BF),
            pltpu.VMEM((256, 512), F32),
            pltpu.VMEM((256, 512), BF),
            pltpu.VMEM((768, 512), BF),
            pltpu.VMEM((2, 512, 512), F32),
            pltpu.VMEM((2, 512, 512), BF),
            pltpu.VMEM((2, 512, 512), BF),
        ],
        compiler_params=pltpu.CompilerParams(vmem_limit_bytes=56 * 1024 * 1024),
        name="coarse",
    )(core, c, cf, ct, ctf, w, ow)


def other_one(v):
    return v + 1 - 2 * (v % 2)


def other_two(v):
    return 3 - v


def tail_kernel(
    ab_ref, arr_ref, pw_ref, c_ref, ct_ref, dn_ref, mix_ref, ow_ref, big,
    out_ref, gof_ref, gp_ref, gq_ref, goc_ref,
    dnf, mixf, small, sm, g, r1, s1, r2, ra, rb, ha, hb, ra2, rb2, z, rz, zf, fa, fb, full,
    send, recv,
):
    rep = lax.axis_index("rep")
    pts = lax.axis_index("pts")
    x = rep % 4
    zlo = rep // 4
    y = pts // 8
    zhi = (pts // 2) % 4
    core = pts % 2
    zi = zhi * 2 + zlo

    def at_x(v):
        return (zlo * 4 + v, pts)

    def at_y(v):
        return (rep, v * 8 + zhi * 2 + core)

    def at_z(v):
        return ((v % 2) * 4 + x, y * 8 + (v // 2) * 2 + core)

    partner = (rep, pts + 1 - 2 * core)
    barrier = pltpu.get_barrier_semaphore()
    peers = [partner]
    peers += [at_x((x + d) % 4) for d in (1, 2, 3)] + [at_y((y + d) % 4) for d in (1, 2, 3)]
    peers += [at_z((zi + d) % 8) for d in range(1, 8)]
    for peer in peers:
        pl.semaphore_signal(barrier, inc=1, device_id=peer, device_id_type=MESH)
    pl.semaphore_wait(barrier, len(peers))

    counter = [0]

    def push(src, dst, peer):
        i = counter[0]
        counter[0] += 1
        copy = pltpu.make_async_remote_copy(
            src_ref=src, dst_ref=dst, send_sem=send.at[i], recv_sem=recv.at[i],
            device_id=peer, device_id_type=MESH,
        )
        copy.start()
        return copy

    def wait(copies):
        for copy in copies:
            copy.wait()

    streams = [
        (x, at_x, 0, other_one, other_two),
        (x, at_x, 64, other_two, other_one),
        (y, at_y, 128, other_one, other_two),
        (y, at_y, 192, other_two, other_one),
    ]

    def quarter(base, v):
        return pl.ds(base + v * 16, 16)

    trade = [push(dn_ref.at[pl.ds(256, 256)], dnf, partner)]
    trade.append(push(mix_ref.at[pl.ds(256, 256)], mixf, partner))
    first = []
    for k, (v, place, base, one, two) in enumerate(streams):
        p = one(v)
        first.append(push(big.at[quarter(base, two(p))], r1.at[k, 1], place(p)))
        first.append(push(big.at[quarter(base, p)], r1.at[k, 0], place(p)))

    c = c_ref[...].astype(F32)
    u, count = pooled_mean(ab_ref, arr_ref, pw_ref)
    th = jnp.tanh(GA * (u + GB * u * u * u))
    slope = 0.5 * (1.0 + th) + 0.5 * u * (1.0 - th * th) * (GA * (1.0 + 3.0 * GB * u * u))
    r = lax.rsqrt(jnp.mean(c * c, axis=-1, keepdims=True) + EPS)
    at = jnp.transpose(pooled(ab_ref, arr_ref, 0, 256)).astype(BF)
    bt = jnp.transpose(pooled(ab_ref, arr_ref, 256, 512)).astype(BF)
    wait(trade)
    dn = dn_ref[:256].astype(F32) + dnf[...].astype(F32)
    inner = jnp.mean(dn * c, axis=-1, keepdims=True)
    dc = r * dn - c * (r * r * r * inner) + ct_ref[...].astype(F32)
    gs = (slope * dc / count).astype(BF)
    gw = mm(gs, pw_ref[...], NT).astype(BF)
    for half in range(2):
        rows = slice(half * 128, half * 128 + 128)
        for j in range(4):
            block = mm(at[rows], gs[:, j * 128 : j * 128 + 128]).astype(BF)
            small[half, j * 8 : j * 8 + 8] = block.reshape(8, 16, 128)
        for j in range(2):
            block = mm(bt[rows], gw[:, j * 128 : j * 128 + 128]).astype(BF)
            small[half, 32 + j * 8 : 40 + j * 8] = block.reshape(8, 16, 128)
    swap = push(small.at[1 - core], sm, partner)

    def f32(value):
        return value.astype(F32)

    second = []
    for k, (v, place, base, one, two) in enumerate(streams):
        wait(first[2 * k : 2 * k + 2])
        s1[k] = (f32(big[quarter(base, two(v))]) + f32(r1[k, 1])).astype(BF)
        second.append(push(s1.at[k], r2.at[k], place(two(v))))
    swap.wait()
    g[:48] = (f32(small[core]) + f32(sm[...])).astype(BF)
    g[48:] = jnp.zeros((16, 16, 128), BF)
    third = []
    for d in (1, 2, 3):
        to = (x + d) % 4
        third.append(push(g.at[pl.ds(to * 8, 8)], ra.at[d - 1], at_x(to)))
        to = (y + d) % 4
        third.append(push(g.at[pl.ds(32 + to * 8, 8)], rb.at[d - 1], at_y(to)))
    lo = pl.multiple_of(core * 256, 256)
    hi = pl.multiple_of(256 - core * 256, 256)
    mixed = mm(mix_ref[:256], ow_ref[pl.ds(lo, 256), :]) + mm(mixf[...], ow_ref[pl.ds(hi, 256), :])
    out_ref[...] = (c + mixed).astype(BF)

    def add(own, slots, n):
        total = f32(own)
        for d in range(n):
            total = total + f32(slots[d])
        return total.astype(BF)

    for k, (v, place, base, one, two) in enumerate(streams):
        second[k].wait()
        total = (f32(big[quarter(base, v)]) + f32(r1[k, 0]) + f32(r2[k])).astype(BF)
        keep = ha if k < 2 else hb
        spot = (k % 2) * 4
        keep[:, spot : spot + 4] = total.reshape(4, 4, 16, 128)
    wait(third)
    ha[:, 8:] = add(g[pl.ds(x * 8, 8)], ra, 3).reshape(4, 2, 16, 128)
    hb[:, 8:] = add(g[pl.ds(32 + y * 8, 8)], rb, 3).reshape(4, 2, 16, 128)
    moves = []
    for d in (1, 2, 3):
        to = (y + d) % 4
        moves.append(push(ha.at[to], ra2.at[d - 1], at_y(to)))
        to = (x + d) % 4
        moves.append(push(hb.at[to], rb2.at[d - 1], at_x(to)))
    wait(moves)
    z[:10] = add(ha[y], ra2, 3)
    z[10:20] = add(hb[x], rb2, 3)
    z[20:] = jnp.zeros((4, 16, 128), BF)
    moves = []
    for d in (4, 3, 5, 2, 6, 1, 7):
        to = (zi + d) % 8
        moves.append(push(z.at[pl.ds(to * 3, 3)], rz.at[d - 1], at_z(to)))
    wait(moves)
    mine = pl.ds(zi * 3, 3)
    zf[mine] = add(z[mine], rz, 7)
    wait([push(zf.at[mine], zf.at[mine], at_z((zi + d) % 8)) for d in (4, 3, 5, 2, 6, 1, 7)])
    fa[y] = zf[:10]
    fb[x] = zf[10:20]
    moves = []
    for d in (1, 2, 3):
        moves.append(push(fa.at[y], fa.at[y], at_y((y + d) % 4)))
        moves.append(push(fb.at[x], fb.at[x], at_x((x + d) % 4)))
    wait(moves)

    def share(rows, peer):
        spot = full.at[core, rows]
        return push(spot, spot, peer)

    ups = []
    first, second, done = [], [], []
    for k, (v, place, base, one, two) in enumerate(streams):
        kept = fa if k < 2 else fb
        spot = (k % 2) * 4
        own = quarter(base, v)
        full[core, own] = kept[:, spot : spot + 4].reshape(16, 16, 128)
        first.append(share(own, place(two(v))))
        second.append(share(own, place(one(v))))
        done.append(share(own, partner))
    la, lb = pl.ds(256 + x * 8, 8), pl.ds(288 + y * 8, 8)
    full[core, la] = fa[:, 8:].reshape(8, 16, 128)
    full[core, lb] = fb[:, 8:].reshape(8, 16, 128)
    for d in (1, 2, 3):
        ups.append(share(la, at_x((x + d) % 4)))
        ups.append(share(lb, at_y((y + d) % 4)))
    for k, (v, place, base, one, two) in enumerate(streams):
        first[k].wait()
        came = quarter(base, two(v))
        second.append(share(came, place(one(v))))
        done.append(share(came, partner))
    wait(ups)
    done.append(share(pl.ds(256, 48), partner))
    for k, (v, place, base, one, two) in enumerate(streams):
        second[k].wait()
        second[4 + k].wait()
        done.append(share(quarter(base, one(v)), partner))
        done.append(share(quarter(base, two(one(v))), partner))
    wait(done)
    for c in range(2):
        for j in range(6):
            column = (j // 2) * 512 + c * 256 + (j % 2) * 128
            gq_ref[:, column : column + 128] = full[c, j * 32 : j * 32 + 32].reshape(512, 128)
        for j in range(4):
            rows = slice(c * 256, c * 256 + 256)
            tile = full[c, 192 + j * 16 : 208 + j * 16].reshape(256, 128)
            goc_ref[rows, j * 128 : j * 128 + 128] = tile
        rows = slice(c * 128, c * 128 + 128)
        for j in range(4):
            tile = full[c, 256 + j * 8 : 264 + j * 8].reshape(128, 128)
            gp_ref[rows, j * 128 : j * 128 + 128] = tile
        for j in range(2):
            tile = full[c, 288 + j * 8 : 296 + j * 8].reshape(128, 128)
            gof_ref[rows, j * 128 : j * 128 + 128] = tile


def tail_call(*operands):
    def tiles(*n):
        return pltpu.VMEM((*n, 16, 128), BF)

    return pl.pallas_call(
        tail_kernel,
        out_shape=(
            jax.ShapeDtypeStruct((256, 512), BF),
            jax.ShapeDtypeStruct((256, 256), BF),
            jax.ShapeDtypeStruct((256, 512), BF),
            jax.ShapeDtypeStruct((512, 1536), BF),
            jax.ShapeDtypeStruct((512, 512), BF),
        ),
        in_specs=[VM] * 9,
        out_specs=(VM,) * 5,
        scratch_shapes=[
            pltpu.VMEM((256, 512), BF), pltpu.VMEM((256, 256), BF),
            tiles(2, 48), tiles(48), tiles(64),
            tiles(4, 2, 16), tiles(4, 16), tiles(4, 16), tiles(3, 8), tiles(3, 8),
            tiles(4, 10), tiles(4, 10), tiles(3, 10), tiles(3, 10),
            tiles(24), tiles(7, 3), tiles(24), tiles(4, 10), tiles(4, 10), tiles(2, 320),
            pltpu.SemaphoreType.DMA((96,)),
            pltpu.SemaphoreType.DMA((96,)),
        ],
        compiler_params=pltpu.CompilerParams(
            collective_id=0, has_side_effects=True, vmem_limit_bytes=40 * 1024 * 1024
        ),
        name="tail",
    )(*operands)


def local(
    fine_points, parent, patch_count, qkv_fine, out_fine, pool_weight, qkv_coarse, out_coarse,
    cotangent,
):
    pts = lax.axis_index("pts")
    position = lax.axis_index("rep") * lax.axis_size("pts") + pts
    core = (pts % 2).reshape(1)
    swap = [(i, i ^ 1) for i in range(32)]
    far_cot = lax.ppermute(cotangent, "pts", swap)
    offset = (parent - position * 256).reshape(1, 1024)
    ab = fine_call(patch_count, offset, fine_points, qkv_fine, out_fine)
    arrived = lax.ppermute(ab[256:], "pts", [(i, i + 1) for i in range(31)])
    coarse_in = pl.pallas_call(
        coarse_in_kernel,
        out_shape=jax.ShapeDtypeStruct((256, 512), BF),
        in_specs=[VM, VM, VM],
        out_specs=VM,
        name="coarse_in",
    )(ab, arrived, pool_weight)
    far_in = lax.ppermute(coarse_in, "pts", swap)
    dn, mixed, big = coarse_call(core, coarse_in, far_in, cotangent, far_cot, qkv_coarse, out_coarse)
    return tail_call(
        ab, arrived, pool_weight, coarse_in, cotangent, dn, mixed, out_coarse, big
    )


def solution(mesh):
    rows = P(("rep", "pts"), None)
    flat = P(("rep", "pts"))
    return jax.shard_map(
        local,
        mesh=mesh,
        in_specs=(rows, flat, flat, P(), P(), P(), P(), P(), rows),
        out_specs=(rows, P(), P(), P(), P()),
        check_vma=False,
    )
```

```python
import jax
import jax.numpy as jnp
from jax import lax
from jax.experimental import pallas as pl
from jax.experimental.pallas import tpu as pltpu
from jax.sharding import PartitionSpec as P

F32 = jnp.float32
BF = jnp.bfloat16
EPS = 1e-6
LOG2E = 1.4426950408889634
LN2 = 0.6931471805599453
SAFE = 80.0
MESH = pl.DeviceIdType.MESH
VM = pl.BlockSpec(memory_space=pltpu.VMEM)
SM = pl.BlockSpec(memory_space=pltpu.SMEM)

NN = (((1,), (0,)), ((), ()))
NT = (((1,), (1,)), ((), ()))
TN = (((0,), (0,)), ((), ()))
TT = (((0,), (1,)), ((), ()))


def mm(a, b, dims=NN):
    return lax.dot_general(a, b, dims, preferred_element_type=F32)


def normalize(values):
    return values * lax.rsqrt(jnp.mean(values * values, axis=-1, keepdims=True) + EPS)


def split_dot(a, b):
    high = a.astype(BF)
    low = (a - high.astype(F32)).astype(BF)
    return mm(high, b) + mm(low, b)


def head_rows(rows, width):
    return lax.broadcasted_iota(jnp.int32, (rows, width), 0) // 16


def score_bound(qt, k):
    channels = qt.shape[0]
    heads = (
        lax.broadcasted_iota(jnp.int32, (channels, 128), 0) // 16
        == lax.broadcasted_iota(jnp.int32, (channels, 128), 1)
    ).astype(BF)
    kf = k.astype(F32)
    k2 = mm((kf * kf).astype(BF), heads)
    q = qt.astype(F32)
    q2 = (q * q).reshape(channels // 16, 16, qt.shape[1]).sum(axis=1)
    return jnp.max(q2) * jnp.max(k2)


def fine_kernel(cnt_ref, off_ref, x_ref, w_ref, ow_ref, ab_ref, k_ref, qt_ref, va_ref, mt_ref):
    count = cnt_ref[0]
    shift = (lax.axis_index("rep") * lax.axis_size("pts") + lax.axis_index("pts")) * 256
    offset = off_ref[...] - shift
    x = x_ref[...]
    n = normalize(x.astype(F32)).astype(BF)
    k_ref[...] = mm(n, w_ref[:, 256:512]).astype(BF)
    qt_ref[...] = (mm(w_ref[:, :256], n, TT) * (0.25 * LOG2E)).astype(BF)
    vt = mm(w_ref[:, 512:], n, TT).astype(BF)
    live = lax.broadcasted_iota(jnp.int32, (1, 1024), 1) < count
    ones = jnp.where(jnp.broadcast_to(live, (16, 1024)), 1.0, 0.0).astype(BF)
    for h in range(16):
        rows = vt[h * 16 : h * 16 + 16, :].astype(F32)
        va_ref[h, 0:16, :] = jnp.where(live, rows, 0.0).astype(BF)
        va_ref[h, 16:32, :] = ones
    bound = score_bound(qt_ref[...], k_ref[...])
    quick = bound < SAFE * SAFE

    def safe_head(h, carry):
        half = pl.multiple_of((h // 8) * 128, 128)
        row = pl.multiple_of(h * 16, 16)
        chosen = head_rows(128, 256) == h % 8
        alive = lax.broadcasted_iota(jnp.int32, (1024, 256), 0) < count
        for t in range(4):
            cols = slice(t * 256, t * 256 + 256)
            part = qt_ref[pl.ds(half, 128), cols]
            s = mm(k_ref[:, pl.ds(half, 128)], jnp.where(chosen, part, jnp.zeros_like(part)))
            s = jnp.where(alive, s, -1e30)
            s = s - jnp.max(s, axis=0, keepdims=True)
            o = mm(va_ref[h], jnp.exp2(s).astype(BF))
            mt_ref[pl.ds(row, 16), cols] = (o[:16] / o[16:]).astype(BF)
        return carry

    def quick_head(h, carry):
        half = pl.multiple_of((h // 8) * 128, 128)
        row = pl.multiple_of(h * 16, 16)
        ck, cq = 1024, 256
        units = [(t, c) for t in range(1024 // cq) for c in range(1024 // ck)]
        chosen = head_rows(128, cq) == h % 8
        scores, weights, sums, queries = {}, {}, {}, {}
        for i in range(len(units) + 2):
            if i < len(units):
                t, c = units[i]
                if c == 0:
                    part = qt_ref[pl.ds(half, 128), t * cq : t * cq + cq]
                    queries[t] = jnp.where(chosen, part, jnp.zeros_like(part))
                scores[i] = mm(k_ref[c * ck : c * ck + ck, pl.ds(half, 128)], queries[t])
            if 1 <= i <= len(units):
                weights[i - 1] = jnp.exp2(scores.pop(i - 1)).astype(BF)
            if i >= 2:
                t, c = units[i - 2]
                o = mm(va_ref[h, :, c * ck : c * ck + ck], weights.pop(i - 2))
                sums[t] = o if c == 0 else sums[t] + o
                if c == 1024 // ck - 1:
                    o = sums.pop(t)
                    mt_ref[pl.ds(row, 16), t * cq : t * cq + cq] = (o[:16] / o[16:]).astype(BF)
        return carry

    @pl.when(quick)
    def _():
        lax.fori_loop(0, 16, quick_head, 0, unroll=4)

    @pl.when(jnp.logical_not(quick))
    def _():
        lax.fori_loop(0, 16, safe_head, 0)

    table = jnp.where(
        (lax.broadcasted_iota(jnp.int32, (288, 1024), 0) == offset) & live, 1.0, 0.0
    )
    total = jnp.sum(table, axis=1, keepdims=True)
    table = table.astype(BF)
    b = mm(table, mt_ref[...], NT)
    ab_ref[:, :256] = mm(table, x) + split_dot(b, ow_ref[...])
    ab_ref[:, 256:512] = b
    ab_ref[:, 512:] = jnp.broadcast_to(total, (288, 128))


def fine_call(count, offset, x, w, ow):
    return pl.pallas_call(
        fine_kernel,
        out_shape=jax.ShapeDtypeStruct((288, 640), F32),
        in_specs=[SM, VM, VM, VM, VM],
        out_specs=VM,
        scratch_shapes=[
            pltpu.VMEM((1024, 256), BF),
            pltpu.VMEM((256, 1024), BF),
            pltpu.VMEM((16, 32, 1024), BF),
            pltpu.VMEM((256, 1024), BF),
        ],
        compiler_params=pltpu.CompilerParams(vmem_limit_bytes=24 * 1024 * 1024),
        name="fine",
    )(count, offset, x, w, ow)


GA = 0.7978845608028654
GB = 0.044715


def pooled_mean(ab_ref, pw_ref):
    count = jnp.maximum(ab_ref[:, 512:513], 1.0)
    return split_dot(ab_ref[:, :256], pw_ref[...]) / count, count


def middle_kernel(
    ab_ref, pw_ref, ct_ref, sum_ref, c_ref, cf_ref, ctf_ref, arrived, send, recv
):
    rep = lax.axis_index("rep")
    pts = lax.axis_index("pts")
    total = lax.axis_size("pts")
    ahead = (rep, (pts + 1) % total)
    behind = (rep, (pts + total - 1) % total)
    partner = (rep, pts + 1 - 2 * (pts % 2))
    barrier = pltpu.get_barrier_semaphore()
    for peer in (ahead, behind, partner):
        pl.semaphore_signal(barrier, inc=1, device_id=peer, device_id_type=MESH)
    pl.semaphore_wait(barrier, 3)

    def push(i, src, dst, peer):
        copy = pltpu.make_async_remote_copy(
            src_ref=src, dst_ref=dst, send_sem=send.at[i], recv_sem=recv.at[i],
            device_id=peer, device_id_type=MESH,
        )
        copy.start()
        return copy

    moved = push(0, ab_ref.at[pl.ds(256, 32)], arrived, ahead)
    cot = push(1, ct_ref, ctf_ref, partner)
    sum_ref[32:] = ab_ref[32:256]
    moved.wait()
    sum_ref[:32] = ab_ref[:32] + arrived[...]
    u, _ = pooled_mean(sum_ref, pw_ref)
    c_ref[...] = (0.5 * u * (1.0 + jnp.tanh(GA * (u + GB * u * u * u)))).astype(BF)
    push(2, c_ref, cf_ref, partner).wait()
    cot.wait()


def middle_call(ab, pw, ct):
    half = jax.ShapeDtypeStruct((256, 512), BF)
    return pl.pallas_call(
        middle_kernel,
        out_shape=(jax.ShapeDtypeStruct((256, 640), F32), half, half, half),
        in_specs=[VM] * 3,
        out_specs=(VM,) * 4,
        scratch_shapes=[
            pltpu.VMEM((32, 640), F32),
            pltpu.SemaphoreType.DMA((3,)),
            pltpu.SemaphoreType.DMA((3,)),
        ],
        compiler_params=pltpu.CompilerParams(
            collective_id=1, has_side_effects=True, vmem_limit_bytes=12 * 1024 * 1024
        ),
        name="middle",
    )(ab, pw, ct)


def coarse_kernel(
    c_ref, cf_ref, ct_ref, ctf_ref, w_ref, ow_ref,
    dn_ref, mix_ref, g_ref,
    n_ref, cot_ref, k_ref, v_ref, kt_ref, qt_ref, va_ref, dot_ref, ot_ref, dp_ref,
    p_ref, pb_ref, ds_ref,
):
    core = lax.axis_index("pts") % 2
    lo = pl.multiple_of(core * 256, 256)
    n_ref[:256] = normalize(c_ref[...].astype(F32)).astype(BF)
    n_ref[256:] = normalize(cf_ref[...].astype(F32)).astype(BF)
    cot_ref[:256] = ct_ref[...]
    cot_ref[256:] = ctf_ref[...]
    n = n_ref[...]
    wq = w_ref[:, pl.ds(lo, 256)]
    wk = w_ref[:, pl.ds(512 + lo, 256)]
    wv = w_ref[:, pl.ds(1024 + lo, 256)]
    qt_ref[...] = (mm(wq, n, TT) * (0.25 * LOG2E)).astype(BF)
    k_ref[...] = mm(n, wk).astype(BF)
    v_ref[...] = mm(n, wv).astype(BF)
    kt_ref[...] = mm(wk, n, TT).astype(BF)
    vt = mm(wv, n, TT).astype(BF)
    for h in range(16):
        va_ref[h, :16, :] = vt[h * 16 : h * 16 + 16, :]
        va_ref[h, 16:, :] = jnp.ones((16, 512), BF)
    dot_ref[...] = mm(ow_ref[pl.ds(lo, 256), :], cot_ref[...], NT)
    quick = score_bound(qt_ref[...], k_ref[...]) < SAFE * SAFE

    def stage_one(h, slot, shift):
        half = pl.multiple_of((h // 8) * 128, 128)
        row = pl.multiple_of(h * 16, 16)
        chosen = head_rows(128, 512) == h % 8
        part = qt_ref[pl.ds(half, 128), :]
        qm = jnp.where(chosen, part, jnp.zeros_like(part))
        s = mm(k_ref[:, pl.ds(half, 128)], qm)
        if shift:
            s = s - jnp.max(s, axis=0, keepdims=True)
        p = jnp.exp2(s)
        p_ref[slot] = p
        pb_ref[slot] = p.astype(BF)

    def stage_two(h, slot):
        half = pl.multiple_of((h // 8) * 128, 128)
        row = pl.multiple_of(h * 16, 16)
        chosen = head_rows(128, 512) == h % 8
        pb = pb_ref[slot]
        o = mm(va_ref[h], pb)
        inverse = 1.0 / o[16:]
        on = o[:16] * inverse
        ot_ref[pl.ds(row, 16), :] = on.astype(BF)
        do = dot_ref[pl.ds(row, 16), :] * inverse
        dob = do.astype(BF)
        delta = jnp.sum(dob.astype(F32) * on, axis=0, keepdims=True)
        tiled = jnp.concatenate([dob] * 8, axis=0)
        dom = jnp.where(chosen, tiled, jnp.zeros_like(tiled))
        dpt = mm(v_ref[:, pl.ds(half, 128)], dom)
        ds_ref[slot] = (p_ref[slot] * (dpt - delta)).astype(BF)
        dp_ref[pl.ds(512 + row, 16), :] = mm(dob, pb, NT).astype(BF)

    def stage_three(h, slot):
        row = pl.multiple_of(h * 16, 16)
        ds = ds_ref[slot]
        dp_ref[pl.ds(row, 16), :] = (mm(kt_ref[pl.ds(row, 16), :], ds) * 0.25).astype(BF)
        dk = mm(qt_ref[pl.ds(row, 16), :], ds, NT) * LN2
        dp_ref[pl.ds(256 + row, 16), :] = dk.astype(BF)

    def attend(shift):
        stage_one(0, 0, shift)
        stage_one(1, 1, shift)
        stage_two(0, 0)

        def step(j, carry):
            for e in (0, 1):
                h = 2 * j + e
                stage_two(h + 1, 1 - e)
                stage_three(h, e)
                stage_one(h + 2, e, shift)
            return carry

        lax.fori_loop(0, 7, step, 0)
        stage_two(15, 1)
        stage_three(14, 0)
        stage_three(15, 1)

    @pl.when(quick)
    def _():
        attend(False)

    @pl.when(jnp.logical_not(quick))
    def _():
        attend(True)

    mix_ref[...] = jnp.transpose(ot_ref[...])
    dnt = (
        mm(wq, dp_ref[:256, :]) + mm(wk, dp_ref[256:512, :]) + mm(wv, dp_ref[512:, :])
    ).astype(BF)
    dn_ref[...] = jnp.transpose(dnt)
    nt = jnp.transpose(n_ref[...])
    for j in range(6):
        block = mm(nt, dp_ref[j * 128 : j * 128 + 128, :], NT).astype(BF)
        g_ref[j * 32 : j * 32 + 32] = block.reshape(32, 16, 128)
    for j in range(4):
        block = mm(ot_ref[...], cot_ref[:, j * 128 : j * 128 + 128]).astype(BF)
        g_ref[192 + j * 16 : 208 + j * 16] = block.reshape(16, 16, 128)


def coarse_call(c, cf, ct, ctf, w, ow):
    return pl.pallas_call(
        coarse_kernel,
        out_shape=(
            jax.ShapeDtypeStruct((512, 512), BF),
            jax.ShapeDtypeStruct((512, 256), BF),
            jax.ShapeDtypeStruct((256, 16, 128), BF),
        ),
        in_specs=[VM] * 6,
        out_specs=(VM, VM, VM),
        scratch_shapes=[
            pltpu.VMEM((512, 512), BF),
            pltpu.VMEM((512, 512), BF),
            pltpu.VMEM((512, 256), BF),
            pltpu.VMEM((512, 256), BF),
            pltpu.VMEM((256, 512), BF),
            pltpu.VMEM((256, 512), BF),
            pltpu.VMEM((16, 32, 512), BF),
            pltpu.VMEM((256, 512), F32),
            pltpu.VMEM((256, 512), BF),
            pltpu.VMEM((768, 512), BF),
            pltpu.VMEM((2, 512, 512), F32),
            pltpu.VMEM((2, 512, 512), BF),
            pltpu.VMEM((2, 512, 512), BF),
        ],
        compiler_params=pltpu.CompilerParams(vmem_limit_bytes=28 * 1024 * 1024),
        name="coarse",
    )(c, cf, ct, ctf, w, ow)


def other_one(v):
    return v + 1 - 2 * (v % 2)


def other_two(v):
    return 3 - v


def tail_kernel(
    ab_ref, pw_ref, c_ref, ct_ref, dn_ref, mix_ref, ow_ref, big,
    out_ref, full,
    dnf, mixf, small, sm, g, r1, s1, r2, ra, rb, ha, hb, ra2, rb2, z, rz, zf, fa, fb,
    send, recv,
):
    rep = lax.axis_index("rep")
    pts = lax.axis_index("pts")
    x = rep % 4
    zlo = rep // 4
    y = pts // 8
    zhi = (pts // 2) % 4
    core = pts % 2
    zi = zhi * 2 + zlo

    def at_x(v):
        return (zlo * 4 + v, pts)

    def at_y(v):
        return (rep, v * 8 + zhi * 2 + core)

    def at_z(v):
        return ((v % 2) * 4 + x, y * 8 + (v // 2) * 2 + core)

    partner = (rep, pts + 1 - 2 * core)
    barrier = pltpu.get_barrier_semaphore()
    peers = [partner]
    peers += [at_x((x + d) % 4) for d in (1, 2, 3)] + [at_y((y + d) % 4) for d in (1, 2, 3)]
    peers += [at_z((zi + d) % 8) for d in range(1, 8)]
    for peer in peers:
        pl.semaphore_signal(barrier, inc=1, device_id=peer, device_id_type=MESH)
    pl.semaphore_wait(barrier, len(peers))

    counter = [0]

    def push(src, dst, peer):
        i = counter[0]
        counter[0] += 1
        copy = pltpu.make_async_remote_copy(
            src_ref=src, dst_ref=dst, send_sem=send.at[i], recv_sem=recv.at[i],
            device_id=peer, device_id_type=MESH,
        )
        copy.start()
        return copy

    def wait(copies):
        for copy in copies:
            copy.wait()

    streams = [
        (x, at_x, 0, other_one, other_two),
        (x, at_x, 64, other_two, other_one),
        (y, at_y, 128, other_one, other_two),
        (y, at_y, 192, other_two, other_one),
    ]

    def quarter(base, v):
        return pl.ds(base + v * 16, 16)

    trade = [push(dn_ref.at[pl.ds(256, 256)], dnf, partner)]
    trade.append(push(mix_ref.at[pl.ds(256, 256)], mixf, partner))
    first = []
    for k, (v, place, base, one, two) in enumerate(streams):
        p = one(v)
        first.append(push(big.at[quarter(base, two(p))], r1.at[k, 1], place(p)))
        first.append(push(big.at[quarter(base, p)], r1.at[k, 0], place(p)))

    c = c_ref[...].astype(F32)
    u, count = pooled_mean(ab_ref, pw_ref)
    th = jnp.tanh(GA * (u + GB * u * u * u))
    slope = 0.5 * (1.0 + th) + 0.5 * u * (1.0 - th * th) * (GA * (1.0 + 3.0 * GB * u * u))
    r = lax.rsqrt(jnp.mean(c * c, axis=-1, keepdims=True) + EPS)
    at = jnp.transpose(ab_ref[:, :256]).astype(BF)
    bt = jnp.transpose(ab_ref[:, 256:512]).astype(BF)
    wait(trade)
    dn = dn_ref[:256].astype(F32) + dnf[...].astype(F32)
    inner = jnp.mean(dn * c, axis=-1, keepdims=True)
    dc = r * dn - c * (r * r * r * inner) + ct_ref[...].astype(F32)
    gs = (slope * dc / count).astype(BF)
    gw = mm(gs, pw_ref[...], NT).astype(BF)
    for half in range(2):
        rows = slice(half * 128, half * 128 + 128)
        for j in range(4):
            block = mm(at[rows], gs[:, j * 128 : j * 128 + 128]).astype(BF)
            small[half, j * 8 : j * 8 + 8] = block.reshape(8, 16, 128)
        for j in range(2):
            block = mm(bt[rows], gw[:, j * 128 : j * 128 + 128]).astype(BF)
            small[half, 32 + j * 8 : 40 + j * 8] = block.reshape(8, 16, 128)
    swap = push(small.at[1 - core], sm, partner)

    def f32(value):
        return value.astype(F32)

    second = []
    for k, (v, place, base, one, two) in enumerate(streams):
        wait(first[2 * k : 2 * k + 2])
        s1[k] = (f32(big[quarter(base, two(v))]) + f32(r1[k, 1])).astype(BF)
        second.append(push(s1.at[k], r2.at[k], place(two(v))))
    swap.wait()
    g[:48] = (f32(small[core]) + f32(sm[...])).astype(BF)
    g[48:] = jnp.zeros((16, 16, 128), BF)
    third = []
    for d in (1, 2, 3):
        to = (x + d) % 4
        third.append(push(g.at[pl.ds(to * 8, 8)], ra.at[d - 1], at_x(to)))
        to = (y + d) % 4
        third.append(push(g.at[pl.ds(32 + to * 8, 8)], rb.at[d - 1], at_y(to)))
    lo = pl.multiple_of(core * 256, 256)
    hi = pl.multiple_of(256 - core * 256, 256)
    mixed = mm(mix_ref[:256], ow_ref[pl.ds(lo, 256), :]) + mm(mixf[...], ow_ref[pl.ds(hi, 256), :])
    out_ref[...] = (c + mixed).astype(BF)

    def add(own, slots, n):
        total = f32(own)
        for d in range(n):
            total = total + f32(slots[d])
        return total.astype(BF)

    for k, (v, place, base, one, two) in enumerate(streams):
        second[k].wait()
        total = (f32(big[quarter(base, v)]) + f32(r1[k, 0]) + f32(r2[k])).astype(BF)
        keep = ha if k < 2 else hb
        spot = (k % 2) * 4
        keep[:, spot : spot + 4] = total.reshape(4, 4, 16, 128)
    wait(third)
    ha[:, 8:] = add(g[pl.ds(x * 8, 8)], ra, 3).reshape(4, 2, 16, 128)
    hb[:, 8:] = add(g[pl.ds(32 + y * 8, 8)], rb, 3).reshape(4, 2, 16, 128)
    moves = []
    for d in (1, 2, 3):
        to = (y + d) % 4
        moves.append(push(ha.at[to], ra2.at[d - 1], at_y(to)))
        to = (x + d) % 4
        moves.append(push(hb.at[to], rb2.at[d - 1], at_x(to)))
    wait(moves)
    z[:10] = add(ha[y], ra2, 3)
    z[10:20] = add(hb[x], rb2, 3)
    z[20:] = jnp.zeros((4, 16, 128), BF)
    moves = []
    for d in (4, 3, 5, 2, 6, 1, 7):
        to = (zi + d) % 8
        moves.append(push(z.at[pl.ds(to * 3, 3)], rz.at[d - 1], at_z(to)))
    wait(moves)
    mine = pl.ds(zi * 3, 3)
    zf[mine] = add(z[mine], rz, 7)
    wait([push(zf.at[mine], zf.at[mine], at_z((zi + d) % 8)) for d in (4, 3, 5, 2, 6, 1, 7)])
    fa[y] = zf[:10]
    fb[x] = zf[10:20]
    moves = []
    for d in (1, 2, 3):
        moves.append(push(fa.at[y], fa.at[y], at_y((y + d) % 4)))
        moves.append(push(fb.at[x], fb.at[x], at_x((x + d) % 4)))
    wait(moves)

    def share(rows, peer):
        spot = full.at[core, rows]
        return push(spot, spot, peer)

    ups = []
    first, second, done = [], [], []
    for k, (v, place, base, one, two) in enumerate(streams):
        kept = fa if k < 2 else fb
        spot = (k % 2) * 4
        own = quarter(base, v)
        full[core, own] = kept[:, spot : spot + 4].reshape(16, 16, 128)
        first.append(share(own, place(two(v))))
        second.append(share(own, place(one(v))))
        done.append(share(own, partner))
    la, lb = pl.ds(256 + x * 8, 8), pl.ds(288 + y * 8, 8)
    full[core, la] = fa[:, 8:].reshape(8, 16, 128)
    full[core, lb] = fb[:, 8:].reshape(8, 16, 128)
    for d in (1, 2, 3):
        ups.append(share(la, at_x((x + d) % 4)))
        ups.append(share(lb, at_y((y + d) % 4)))
    for k, (v, place, base, one, two) in enumerate(streams):
        first[k].wait()
        came = quarter(base, two(v))
        second.append(share(came, place(one(v))))
        done.append(share(came, partner))
    wait(ups)
    done.append(share(pl.ds(256, 48), partner))
    for k, (v, place, base, one, two) in enumerate(streams):
        second[k].wait()
        second[4 + k].wait()
        done.append(share(quarter(base, one(v)), partner))
        done.append(share(quarter(base, two(one(v))), partner))
    wait(done)


def unpack_kernel(out_ref, full, copy_ref, gof_ref, gp_ref, gq_ref, goc_ref):
    copy_ref[...] = out_ref[...]
    for c in range(2):
        for j in range(6):
            column = (j // 2) * 512 + c * 256 + (j % 2) * 128
            gq_ref[:, column : column + 128] = full[c, j * 32 : j * 32 + 32].reshape(512, 128)
        for j in range(4):
            rows = slice(c * 256, c * 256 + 256)
            tile = full[c, 192 + j * 16 : 208 + j * 16].reshape(256, 128)
            goc_ref[rows, j * 128 : j * 128 + 128] = tile
        rows = slice(c * 128, c * 128 + 128)
        for j in range(4):
            tile = full[c, 256 + j * 8 : 264 + j * 8].reshape(128, 128)
            gp_ref[rows, j * 128 : j * 128 + 128] = tile
        for j in range(2):
            tile = full[c, 288 + j * 8 : 296 + j * 8].reshape(128, 128)
            gof_ref[rows, j * 128 : j * 128 + 128] = tile


def tail_call(*operands):
    def tiles(*n):
        return pltpu.VMEM((*n, 16, 128), BF)

    return pl.pallas_call(
        tail_kernel,
        out_shape=(
            jax.ShapeDtypeStruct((256, 512), BF),
            jax.ShapeDtypeStruct((2, 320, 16, 128), BF),
        ),
        in_specs=[VM] * 8,
        out_specs=(VM,) * 2,
        scratch_shapes=[
            pltpu.VMEM((256, 512), BF), pltpu.VMEM((256, 256), BF),
            tiles(2, 48), tiles(48), tiles(64),
            tiles(4, 2, 16), tiles(4, 16), tiles(4, 16), tiles(3, 8), tiles(3, 8),
            tiles(4, 10), tiles(4, 10), tiles(3, 10), tiles(3, 10),
            tiles(24), tiles(7, 3), tiles(24), tiles(4, 10), tiles(4, 10),
            pltpu.SemaphoreType.DMA((96,)),
            pltpu.SemaphoreType.DMA((96,)),
        ],
        compiler_params=pltpu.CompilerParams(
            collective_id=0, has_side_effects=True, vmem_limit_bytes=20 * 1024 * 1024
        ),
        name="tail",
    )(*operands)


def unpack_call(out, full):
    return pl.pallas_call(
        unpack_kernel,
        out_shape=(
            jax.ShapeDtypeStruct((256, 512), BF),
            jax.ShapeDtypeStruct((256, 256), BF),
            jax.ShapeDtypeStruct((256, 512), BF),
            jax.ShapeDtypeStruct((512, 1536), BF),
            jax.ShapeDtypeStruct((512, 512), BF),
        ),
        in_specs=[VM] * 2,
        out_specs=(VM,) * 5,
        compiler_params=pltpu.CompilerParams(vmem_limit_bytes=12 * 1024 * 1024),
        name="unpack",
    )(out, full)


def local(
    fine_points, parent, patch_count, qkv_fine, out_fine, pool_weight, qkv_coarse, out_coarse,
    cotangent,
):
    ab = fine_call(patch_count, parent.reshape(1, 1024), fine_points, qkv_fine, out_fine)
    sums, coarse_in, far_in, far_cot = middle_call(ab, pool_weight, cotangent)
    dn, mixed, big = coarse_call(coarse_in, far_in, cotangent, far_cot, qkv_coarse, out_coarse)
    return unpack_call(
        *tail_call(sums, pool_weight, coarse_in, cotangent, dn, mixed, out_coarse, big)
    )


def solution(mesh):
    rows = P(("rep", "pts"), None)
    flat = P(("rep", "pts"))
    return jax.shard_map(
        local,
        mesh=mesh,
        in_specs=(rows, flat, flat, P(), P(), P(), P(), P(), rows),
        out_specs=(rows, P(), P(), P(), P()),
        check_vma=False,
    )
```

```python
import jax
import jax.numpy as jnp
from jax import lax
from jax.experimental import pallas as pl
from jax.experimental.pallas import tpu as pltpu
from jax.sharding import PartitionSpec as P

F32 = jnp.float32
BF = jnp.bfloat16
EPS = 1e-6
LOG2E = 1.4426950408889634
LN2 = 0.6931471805599453
SAFE = 80.0
MESH = pl.DeviceIdType.MESH
VM = pl.BlockSpec(memory_space=pltpu.VMEM)
SM = pl.BlockSpec(memory_space=pltpu.SMEM)

NN = (((1,), (0,)), ((), ()))
NT = (((1,), (1,)), ((), ()))
TN = (((0,), (0,)), ((), ()))
TT = (((0,), (1,)), ((), ()))


def mm(a, b, dims=NN):
    return lax.dot_general(a, b, dims, preferred_element_type=F32)


def normalize(values):
    return values * lax.rsqrt(jnp.mean(values * values, axis=-1, keepdims=True) + EPS)


def split_dot(a, b):
    high = a.astype(BF)
    low = (a - high.astype(F32)).astype(BF)
    return mm(high, b) + mm(low, b)


def head_rows(rows, width):
    return lax.broadcasted_iota(jnp.int32, (rows, width), 0) // 16


def score_bound(qt, k):
    channels = qt.shape[0]
    heads = (
        lax.broadcasted_iota(jnp.int32, (channels, 128), 0) // 16
        == lax.broadcasted_iota(jnp.int32, (channels, 128), 1)
    ).astype(BF)
    kf = k.astype(F32)
    k2 = mm((kf * kf).astype(BF), heads)
    q = qt.astype(F32)
    q2 = (q * q).reshape(channels // 16, 16, qt.shape[1]).sum(axis=1)
    return jnp.max(q2) * jnp.max(k2)


def fine_kernel(
    cnt_ref, off_hbm, x_hbm, w_hbm, ow_hbm, ab_ref,
    k_ref, qt_ref, va_ref, mt_ref, off_ref, x_ref, w_ref, ow_ref, load,
):
    pairs = ((x_hbm, x_ref), (w_hbm, w_ref), (off_hbm, off_ref), (ow_hbm, ow_ref))
    loads = [pltpu.make_async_copy(a, b, load.at[i]) for i, (a, b) in enumerate(pairs)]
    for copy in loads:
        copy.start()
    count = cnt_ref[0]
    shift = (lax.axis_index("rep") * lax.axis_size("pts") + lax.axis_index("pts")) * 256
    loads[0].wait()
    x = x_ref[...]
    n = normalize(x.astype(F32)).astype(BF)
    loads[1].wait()
    loads[2].wait()
    loads[3].wait()
    offset = off_ref[...] - shift
    k_ref[...] = mm(n, w_ref[:, 256:512]).astype(BF)
    qt_ref[...] = (mm(w_ref[:, :256], n, TT) * (0.25 * LOG2E)).astype(BF)
    vt = mm(w_ref[:, 512:], n, TT).astype(BF)
    live = lax.broadcasted_iota(jnp.int32, (1, 1024), 1) < count
    ones = jnp.where(jnp.broadcast_to(live, (16, 1024)), 1.0, 0.0).astype(BF)
    for h in range(16):
        rows = vt[h * 16 : h * 16 + 16, :].astype(F32)
        va_ref[h, 0:16, :] = jnp.where(live, rows, 0.0).astype(BF)
        va_ref[h, 16:32, :] = ones
    bound = score_bound(qt_ref[...], k_ref[...])
    quick = bound < SAFE * SAFE

    def safe_head(h, carry):
        half = pl.multiple_of((h // 8) * 128, 128)
        row = pl.multiple_of(h * 16, 16)
        chosen = head_rows(128, 256) == h % 8
        alive = lax.broadcasted_iota(jnp.int32, (1024, 256), 0) < count
        for t in range(4):
            cols = slice(t * 256, t * 256 + 256)
            part = qt_ref[pl.ds(half, 128), cols]
            s = mm(k_ref[:, pl.ds(half, 128)], jnp.where(chosen, part, jnp.zeros_like(part)))
            s = jnp.where(alive, s, -1e30)
            s = s - jnp.max(s, axis=0, keepdims=True)
            o = mm(va_ref[h], jnp.exp2(s).astype(BF))
            mt_ref[pl.ds(row, 16), cols] = (o[:16] / o[16:]).astype(BF)
        return carry

    def quick_head(h, carry):
        half = pl.multiple_of((h // 8) * 128, 128)
        row = pl.multiple_of(h * 16, 16)
        ck, cq = 1024, 256
        units = [(t, c) for t in range(1024 // cq) for c in range(1024 // ck)]
        chosen = head_rows(128, cq) == h % 8
        scores, weights, sums, queries = {}, {}, {}, {}
        for i in range(len(units) + 2):
            if i < len(units):
                t, c = units[i]
                if c == 0:
                    part = qt_ref[pl.ds(half, 128), t * cq : t * cq + cq]
                    queries[t] = jnp.where(chosen, part, jnp.zeros_like(part))
                scores[i] = mm(k_ref[c * ck : c * ck + ck, pl.ds(half, 128)], queries[t])
            if 1 <= i <= len(units):
                weights[i - 1] = jnp.exp2(scores.pop(i - 1)).astype(BF)
            if i >= 2:
                t, c = units[i - 2]
                o = mm(va_ref[h, :, c * ck : c * ck + ck], weights.pop(i - 2))
                sums[t] = o if c == 0 else sums[t] + o
                if c == 1024 // ck - 1:
                    o = sums.pop(t)
                    mt_ref[pl.ds(row, 16), t * cq : t * cq + cq] = (o[:16] / o[16:]).astype(BF)
        return carry

    @pl.when(quick)
    def _():
        lax.fori_loop(0, 16, quick_head, 0, unroll=4)

    @pl.when(jnp.logical_not(quick))
    def _():
        lax.fori_loop(0, 16, safe_head, 0)

    table = jnp.where(
        (lax.broadcasted_iota(jnp.int32, (288, 1024), 0) == offset) & live, 1.0, 0.0
    )
    total = jnp.sum(table, axis=1, keepdims=True)
    table = table.astype(BF)
    b = mm(table, mt_ref[...], NT)
    ab_ref[:, :256] = mm(table, x) + split_dot(b, ow_ref[...])
    ab_ref[:, 256:512] = b
    ab_ref[:, 512:] = jnp.broadcast_to(total, (288, 128))


def fine_call(count, offset, x, w, ow):
    return pl.pallas_call(
        fine_kernel,
        out_shape=jax.ShapeDtypeStruct((288, 640), F32),
        in_specs=[SM] + [pl.BlockSpec(memory_space=pltpu.HBM)] * 4,
        out_specs=VM,
        scratch_shapes=[
            pltpu.VMEM((1024, 256), BF),
            pltpu.VMEM((256, 1024), BF),
            pltpu.VMEM((16, 32, 1024), BF),
            pltpu.VMEM((256, 1024), BF),
            pltpu.VMEM((1, 1024), jnp.int32),
            pltpu.VMEM((1024, 256), BF),
            pltpu.VMEM((256, 768), BF),
            pltpu.VMEM((256, 256), BF),
            pltpu.SemaphoreType.DMA((4,)),
        ],
        compiler_params=pltpu.CompilerParams(vmem_limit_bytes=24 * 1024 * 1024),
        name="fine",
    )(count, offset, x, w, ow)


GA = 0.7978845608028654
GB = 0.044715


def pooled_mean(sums, pw_ref):
    count = jnp.maximum(sums[:, 512:513], 1.0)
    return split_dot(sums[:, :256], pw_ref[...]) / count, count


def gelu(u):
    return 0.5 * u * (1.0 + jnp.tanh(GA * (u + GB * u * u * u)))


def middle_kernel(
    ab_ref, pw_ref, ct_ref, sum_ref, c_ref, cf_ref, ctf_ref, arrived, send, recv
):
    rep = lax.axis_index("rep")
    pts = lax.axis_index("pts")
    total = lax.axis_size("pts")
    ahead = (rep, (pts + 1) % total)
    behind = (rep, (pts + total - 1) % total)
    partner = (rep, pts + 1 - 2 * (pts % 2))
    barrier = pltpu.get_barrier_semaphore()
    for peer in (ahead, behind, partner):
        pl.semaphore_signal(barrier, inc=1, device_id=peer, device_id_type=MESH)
    own, _ = pooled_mean(ab_ref[32:256], pw_ref)
    sum_ref[32:] = ab_ref[32:256]
    c_ref[32:] = gelu(own).astype(BF)
    pl.semaphore_wait(barrier, 3)

    def push(i, src, dst, peer):
        copy = pltpu.make_async_remote_copy(
            src_ref=src, dst_ref=dst, send_sem=send.at[i], recv_sem=recv.at[i],
            device_id=peer, device_id_type=MESH,
        )
        copy.start()
        return copy

    moved = push(0, ab_ref.at[pl.ds(256, 32)], arrived, ahead)
    cot = push(1, ct_ref, ctf_ref, partner)
    rest = push(2, c_ref.at[pl.ds(32, 224)], cf_ref.at[pl.ds(32, 224)], partner)
    moved.wait()
    first = ab_ref[:32] + arrived[...]
    sum_ref[:32] = first
    u, _ = pooled_mean(first, pw_ref)
    c_ref[:32] = gelu(u).astype(BF)
    last = push(3, c_ref.at[pl.ds(0, 32)], cf_ref.at[pl.ds(0, 32)], partner)
    cot.wait()
    rest.wait()
    last.wait()


def middle_call(ab, pw, ct):
    half = jax.ShapeDtypeStruct((256, 512), BF)
    return pl.pallas_call(
        middle_kernel,
        out_shape=(jax.ShapeDtypeStruct((256, 640), F32), half, half, half),
        in_specs=[VM] * 3,
        out_specs=(VM,) * 4,
        scratch_shapes=[
            pltpu.VMEM((32, 640), F32),
            pltpu.SemaphoreType.DMA((4,)),
            pltpu.SemaphoreType.DMA((4,)),
        ],
        compiler_params=pltpu.CompilerParams(
            collective_id=1, has_side_effects=True, vmem_limit_bytes=12 * 1024 * 1024
        ),
        name="middle",
    )(ab, pw, ct)


def coarse_kernel(
    c_ref, cf_ref, ct_ref, ctf_ref, w_ref, ow_ref,
    dn_ref, mix_ref, g_ref,
    n_ref, cot_ref, k_ref, v_ref, kt_ref, qt_ref, va_ref, dot_ref, ot_ref, dp_ref,
    p_ref, pb_ref, ds_ref,
):
    core = lax.axis_index("pts") % 2
    lo = pl.multiple_of(core * 256, 256)
    n_ref[:256] = normalize(c_ref[...].astype(F32)).astype(BF)
    n_ref[256:] = normalize(cf_ref[...].astype(F32)).astype(BF)
    cot_ref[:256] = ct_ref[...]
    cot_ref[256:] = ctf_ref[...]
    n = n_ref[...]
    wq = w_ref[:, pl.ds(lo, 256)]
    wk = w_ref[:, pl.ds(512 + lo, 256)]
    wv = w_ref[:, pl.ds(1024 + lo, 256)]
    qt_ref[...] = (mm(wq, n, TT) * (0.25 * LOG2E)).astype(BF)
    k_ref[...] = mm(n, wk).astype(BF)
    v_ref[...] = mm(n, wv).astype(BF)
    kt_ref[...] = mm(wk, n, TT).astype(BF)
    vt = mm(wv, n, TT).astype(BF)
    for h in range(16):
        va_ref[h, :16, :] = vt[h * 16 : h * 16 + 16, :]
        va_ref[h, 16:, :] = jnp.ones((16, 512), BF)
    dot_ref[...] = mm(ow_ref[pl.ds(lo, 256), :], cot_ref[...], NT)
    quick = score_bound(qt_ref[...], k_ref[...]) < SAFE * SAFE

    def stage_one(h, slot, shift):
        half = pl.multiple_of((h // 8) * 128, 128)
        row = pl.multiple_of(h * 16, 16)
        chosen = head_rows(128, 512) == h % 8
        part = qt_ref[pl.ds(half, 128), :]
        qm = jnp.where(chosen, part, jnp.zeros_like(part))
        s = mm(k_ref[:, pl.ds(half, 128)], qm)
        if shift:
            s = s - jnp.max(s, axis=0, keepdims=True)
        p = jnp.exp2(s)
        p_ref[slot] = p
        pb_ref[slot] = p.astype(BF)

    def stage_two(h, slot):
        half = pl.multiple_of((h // 8) * 128, 128)
        row = pl.multiple_of(h * 16, 16)
        chosen = head_rows(128, 512) == h % 8
        pb = pb_ref[slot]
        o = mm(va_ref[h], pb)
        inverse = 1.0 / o[16:]
        on = o[:16] * inverse
        ot_ref[pl.ds(row, 16), :] = on.astype(BF)
        do = dot_ref[pl.ds(row, 16), :] * inverse
        dob = do.astype(BF)
        delta = jnp.sum(dob.astype(F32) * on, axis=0, keepdims=True)
        tiled = jnp.concatenate([dob] * 8, axis=0)
        dom = jnp.where(chosen, tiled, jnp.zeros_like(tiled))
        dpt = mm(v_ref[:, pl.ds(half, 128)], dom)
        ds_ref[slot] = (p_ref[slot] * (dpt - delta)).astype(BF)
        dp_ref[pl.ds(512 + row, 16), :] = mm(dob, pb, NT).astype(BF)

    def stage_three(h, slot):
        row = pl.multiple_of(h * 16, 16)
        ds = ds_ref[slot]
        dp_ref[pl.ds(row, 16), :] = (mm(kt_ref[pl.ds(row, 16), :], ds) * 0.25).astype(BF)
        dk = mm(qt_ref[pl.ds(row, 16), :], ds, NT) * LN2
        dp_ref[pl.ds(256 + row, 16), :] = dk.astype(BF)

    def attend(shift):
        stage_one(0, 0, shift)
        stage_one(1, 1, shift)
        stage_two(0, 0)

        def step(j, carry):
            for e in (0, 1):
                h = 2 * j + e
                stage_two(h + 1, 1 - e)
                stage_three(h, e)
                stage_one(h + 2, e, shift)
            return carry

        lax.fori_loop(0, 7, step, 0)
        stage_two(15, 1)
        stage_three(14, 0)
        stage_three(15, 1)

    @pl.when(quick)
    def _():
        attend(False)

    @pl.when(jnp.logical_not(quick))
    def _():
        attend(True)

    mix_ref[...] = jnp.transpose(ot_ref[...])
    dnt = (
        mm(wq, dp_ref[:256, :]) + mm(wk, dp_ref[256:512, :]) + mm(wv, dp_ref[512:, :])
    ).astype(BF)
    dn_ref[...] = jnp.transpose(dnt)
    nt = jnp.transpose(n_ref[...])
    for j in range(6):
        block = mm(nt, dp_ref[j * 128 : j * 128 + 128, :], NT).astype(BF)
        g_ref[j * 32 : j * 32 + 32] = block.reshape(32, 16, 128)
    for j in range(4):
        block = mm(ot_ref[...], cot_ref[:, j * 128 : j * 128 + 128]).astype(BF)
        g_ref[192 + j * 16 : 208 + j * 16] = block.reshape(16, 16, 128)


def coarse_call(c, cf, ct, ctf, w, ow):
    return pl.pallas_call(
        coarse_kernel,
        out_shape=(
            jax.ShapeDtypeStruct((512, 512), BF),
            jax.ShapeDtypeStruct((512, 256), BF),
            jax.ShapeDtypeStruct((256, 16, 128), BF),
        ),
        in_specs=[VM] * 6,
        out_specs=(VM, VM, VM),
        scratch_shapes=[
            pltpu.VMEM((512, 512), BF),
            pltpu.VMEM((512, 512), BF),
            pltpu.VMEM((512, 256), BF),
            pltpu.VMEM((512, 256), BF),
            pltpu.VMEM((256, 512), BF),
            pltpu.VMEM((256, 512), BF),
            pltpu.VMEM((16, 32, 512), BF),
            pltpu.VMEM((256, 512), F32),
            pltpu.VMEM((256, 512), BF),
            pltpu.VMEM((768, 512), BF),
            pltpu.VMEM((2, 512, 512), F32),
            pltpu.VMEM((2, 512, 512), BF),
            pltpu.VMEM((2, 512, 512), BF),
        ],
        compiler_params=pltpu.CompilerParams(vmem_limit_bytes=28 * 1024 * 1024),
        name="coarse",
    )(c, cf, ct, ctf, w, ow)


def other_one(v):
    return v + 1 - 2 * (v % 2)


def other_two(v):
    return 3 - v


def tail_kernel(
    ab_ref, pw_ref, c_ref, ct_ref, dn_ref, mix_ref, ow_ref, big,
    out_ref, full,
    dnf, mixf, slope_ref, at_ref, bt_ref, small, sm, g, r1, s1, r2, ra, rb,
    ha, hb, ra2, rb2, z, rz, zf, fa, fb, send, recv,
):
    rep = lax.axis_index("rep")
    pts = lax.axis_index("pts")
    x = rep % 4
    zlo = rep // 4
    y = pts // 8
    zhi = (pts // 2) % 4
    core = pts % 2
    zi = zhi * 2 + zlo

    def at_x(v):
        return (zlo * 4 + v, pts)

    def at_y(v):
        return (rep, v * 8 + zhi * 2 + core)

    def at_z(v):
        return ((v % 2) * 4 + x, y * 8 + (v // 2) * 2 + core)

    partner = (rep, pts + 1 - 2 * core)
    barrier = pltpu.get_barrier_semaphore()
    peers = [partner]
    peers += [at_x((x + d) % 4) for d in (1, 2, 3)] + [at_y((y + d) % 4) for d in (1, 2, 3)]
    peers += [at_z((zi + d) % 8) for d in range(1, 8)]
    for peer in peers:
        pl.semaphore_signal(barrier, inc=1, device_id=peer, device_id_type=MESH)
    c = c_ref[...].astype(F32)
    u, count = pooled_mean(ab_ref[...], pw_ref)
    th = jnp.tanh(GA * (u + GB * u * u * u))
    slope = 0.5 * (1.0 + th) + 0.5 * u * (1.0 - th * th) * (GA * (1.0 + 3.0 * GB * u * u))
    slope_ref[...] = slope / count
    r = lax.rsqrt(jnp.mean(c * c, axis=-1, keepdims=True) + EPS)
    at_ref[...] = jnp.transpose(ab_ref[:, :256]).astype(BF)
    bt_ref[...] = jnp.transpose(ab_ref[:, 256:512]).astype(BF)
    pl.semaphore_wait(barrier, len(peers))

    counter = [0]

    def push(src, dst, peer):
        i = counter[0]
        counter[0] += 1
        copy = pltpu.make_async_remote_copy(
            src_ref=src, dst_ref=dst, send_sem=send.at[i], recv_sem=recv.at[i],
            device_id=peer, device_id_type=MESH,
        )
        copy.start()
        return copy

    def share(rows, peer):
        spot = full.at[core, rows]
        return push(spot, spot, peer)

    def wait(copies):
        for copy in copies:
            copy.wait()

    def f32(value):
        return value.astype(F32)

    def add(own, slots):
        total = f32(own)
        for slot in slots:
            total = total + f32(slot)
        return total.astype(BF)

    def quarter(base, v):
        return pl.ds(base + v * 8, 8)

    third, done = [], []

    def chain(m):
        streams = [
            (x, at_x, m * 128, other_one, other_two),
            (x, at_x, m * 128 + 32, other_two, other_one),
            (y, at_y, m * 128 + 64, other_one, other_two),
            (y, at_y, m * 128 + 96, other_two, other_one),
        ]
        n = 4 + 2 * m
        w = 1 + m
        some = pl.ds(0, n)
        few = pl.ds(0, w)
        first = []
        for k, (v, place, base, one, two) in enumerate(streams):
            p = one(v)
            first.append(push(big.at[quarter(base, two(p))], r1.at[m, k, 1], place(p)))
            first.append(push(big.at[quarter(base, p)], r1.at[m, k, 0], place(p)))
        yield
        second = []
        for k, (v, place, base, one, two) in enumerate(streams):
            wait(first[2 * k : 2 * k + 2])
            s1[m, k] = add(big[quarter(base, two(v))], [r1[m, k, 1]])
            second.append(push(s1.at[m, k], r2.at[m, k], place(two(v))))
        yield
        for k, (v, place, base, one, two) in enumerate(streams):
            second[k].wait()
            total = add(big[quarter(base, v)], [r1[m, k, 0], r2[m, k]])
            keep = ha if k < 2 else hb
            spot = (k % 2) * 2
            keep[m, :, spot : spot + 2] = total.reshape(4, 2, 16, 128)
        if m:
            wait(third)
            total = add(g[pl.ds(x * 8, 8)], [ra[d] for d in range(3)])
            ha[m, :, 4:] = total.reshape(4, 2, 16, 128)
            total = add(g[pl.ds(32 + y * 8, 8)], [rb[d] for d in range(3)])
            hb[m, :, 4:] = total.reshape(4, 2, 16, 128)
        moves = []
        for d in (2, 1, 3):
            to = (y + d) % 4
            moves.append(push(ha.at[m, to, some], ra2.at[m, d - 1, some], at_y(to)))
            to = (x + d) % 4
            moves.append(push(hb.at[m, to, some], rb2.at[m, d - 1, some], at_x(to)))
        yield
        wait(moves)
        z[m, :n] = add(ha[m, y, :n], [ra2[m, d, :n] for d in range(3)])
        z[m, n : 2 * n] = add(hb[m, x, :n], [rb2[m, d, :n] for d in range(3)])
        if m:
            z[m, 12:] = jnp.zeros((4, 16, 128), BF)
        moves = []
        for d in (4, 3, 5, 2, 6, 1, 7):
            to = (zi + d) % 8
            moves.append(push(z.at[m, pl.ds(to * w, w)], rz.at[m, d - 1, few], at_z(to)))
        yield
        wait(moves)
        mine = pl.ds(zi * w, w)
        zf[m, mine] = add(z[m, mine], [rz[m, d, :w] for d in range(7)])
        spot = zf.at[m, mine]
        moves = [push(spot, spot, at_z((zi + d) % 8)) for d in (4, 3, 5, 2, 6, 1, 7)]
        yield
        wait(moves)
        fa[m, y, :n] = zf[m, :n]
        fb[m, x, :n] = zf[m, n : 2 * n]
        moves = []
        for d in (2, 1, 3):
            spot = fa.at[m, y, some]
            moves.append(push(spot, spot, at_y((y + d) % 4)))
            spot = fb.at[m, x, some]
            moves.append(push(spot, spot, at_x((x + d) % 4)))
        yield
        wait(moves)
        first, second, ups = [], [], []
        for k, (v, place, base, one, two) in enumerate(streams):
            kept = fa if k < 2 else fb
            spot = (k % 2) * 2
            own = quarter(base, v)
            full[core, own] = kept[m, :, spot : spot + 2].reshape(8, 16, 128)
            first.append(share(own, place(two(v))))
            second.append(share(own, place(one(v))))
            done.append(share(own, partner))
        if m:
            la, lb = pl.ds(256 + x * 8, 8), pl.ds(288 + y * 8, 8)
            full[core, la] = fa[m, :, 4:].reshape(8, 16, 128)
            full[core, lb] = fb[m, :, 4:].reshape(8, 16, 128)
            for d in (2, 1, 3):
                ups.append(share(la, at_x((x + d) % 4)))
                ups.append(share(lb, at_y((y + d) % 4)))
        yield
        for k, (v, place, base, one, two) in enumerate(streams):
            first[k].wait()
            came = quarter(base, two(v))
            second.append(share(came, place(one(v))))
            done.append(share(came, partner))
        yield
        if m:
            wait(ups)
            done.append(share(pl.ds(256, 48), partner))
        for k, (v, place, base, one, two) in enumerate(streams):
            second[k].wait()
            second[4 + k].wait()
            done.append(share(quarter(base, one(v)), partner))
            done.append(share(quarter(base, two(one(v))), partner))

    trade = [push(dn_ref.at[pl.ds(256, 256)], dnf, partner)]
    trade.append(push(mix_ref.at[pl.ds(256, 256)], mixf, partner))
    halves = [chain(0), chain(1)]
    next(halves[0])
    next(halves[1])
    wait(trade)
    dn = f32(dn_ref[:256]) + f32(dnf[...])
    inner = jnp.mean(dn * c, axis=-1, keepdims=True)
    dc = r * dn - c * (r * r * r * inner) + f32(ct_ref[...])
    gs = (slope_ref[...] * dc).astype(BF)
    gw = mm(gs, pw_ref[...], NT).astype(BF)
    for half in range(2):
        rows = slice(half * 128, half * 128 + 128)
        for j in range(4):
            block = mm(at_ref[rows], gs[:, j * 128 : j * 128 + 128]).astype(BF)
            small[half, j * 8 : j * 8 + 8] = block.reshape(8, 16, 128)
        for j in range(2):
            block = mm(bt_ref[rows], gw[:, j * 128 : j * 128 + 128]).astype(BF)
            small[half, 32 + j * 8 : 40 + j * 8] = block.reshape(8, 16, 128)
    swap = push(small.at[1 - core], sm, partner)
    next(halves[0])
    swap.wait()
    g[:48] = add(small[core], [sm[...]])
    g[48:] = jnp.zeros((16, 16, 128), BF)
    next(halves[1])
    for d in (2, 1, 3):
        to = (x + d) % 4
        third.append(push(g.at[pl.ds(to * 8, 8)], ra.at[d - 1], at_x(to)))
        to = (y + d) % 4
        third.append(push(g.at[pl.ds(32 + to * 8, 8)], rb.at[d - 1], at_y(to)))
    next(halves[0])
    lo = pl.multiple_of(core * 256, 256)
    hi = pl.multiple_of(256 - core * 256, 256)
    mixed = mm(mix_ref[:256], ow_ref[pl.ds(lo, 256), :]) + mm(mixf[...], ow_ref[pl.ds(hi, 256), :])
    out_ref[...] = (f32(c_ref[...]) + mixed).astype(BF)
    next(halves[1])
    for _ in range(7):
        for half in halves:
            next(half, None)
    wait(done)


def unpack_kernel(out_ref, full, copy_ref, gof_ref, gp_ref, gq_ref, goc_ref):
    copy_ref[...] = out_ref[...]
    for c in range(2):
        for j in range(6):
            column = (j // 2) * 512 + c * 256 + (j % 2) * 128
            gq_ref[:, column : column + 128] = full[c, j * 32 : j * 32 + 32].reshape(512, 128)
        for j in range(4):
            rows = slice(c * 256, c * 256 + 256)
            tile = full[c, 192 + j * 16 : 208 + j * 16].reshape(256, 128)
            goc_ref[rows, j * 128 : j * 128 + 128] = tile
        rows = slice(c * 128, c * 128 + 128)
        for j in range(4):
            tile = full[c, 256 + j * 8 : 264 + j * 8].reshape(128, 128)
            gp_ref[rows, j * 128 : j * 128 + 128] = tile
        for j in range(2):
            tile = full[c, 288 + j * 8 : 296 + j * 8].reshape(128, 128)
            gof_ref[rows, j * 128 : j * 128 + 128] = tile


def tail_call(*operands):
    def tiles(*n):
        return pltpu.VMEM((*n, 16, 128), BF)

    return pl.pallas_call(
        tail_kernel,
        out_shape=(
            jax.ShapeDtypeStruct((256, 512), BF),
            jax.ShapeDtypeStruct((2, 320, 16, 128), BF),
        ),
        in_specs=[VM] * 8,
        out_specs=(VM,) * 2,
        scratch_shapes=[
            pltpu.VMEM((256, 512), BF), pltpu.VMEM((256, 256), BF),
            pltpu.VMEM((256, 512), F32), pltpu.VMEM((256, 256), BF), pltpu.VMEM((256, 256), BF),
            tiles(2, 48), tiles(48), tiles(64),
            tiles(2, 4, 2, 8), tiles(2, 4, 8), tiles(2, 4, 8), tiles(3, 8), tiles(3, 8),
            tiles(2, 4, 6), tiles(2, 4, 6), tiles(2, 3, 6), tiles(2, 3, 6),
            tiles(2, 16), tiles(2, 7, 2), tiles(2, 16), tiles(2, 4, 6), tiles(2, 4, 6),
            pltpu.SemaphoreType.DMA((150,)),
            pltpu.SemaphoreType.DMA((150,)),
        ],
        compiler_params=pltpu.CompilerParams(
            collective_id=0, has_side_effects=True, vmem_limit_bytes=20 * 1024 * 1024
        ),
        name="tail",
    )(*operands)


def unpack_call(out, full):
    return pl.pallas_call(
        unpack_kernel,
        out_shape=(
            jax.ShapeDtypeStruct((256, 512), BF),
            jax.ShapeDtypeStruct((256, 256), BF),
            jax.ShapeDtypeStruct((256, 512), BF),
            jax.ShapeDtypeStruct((512, 1536), BF),
            jax.ShapeDtypeStruct((512, 512), BF),
        ),
        in_specs=[VM] * 2,
        out_specs=(VM,) * 5,
        compiler_params=pltpu.CompilerParams(vmem_limit_bytes=12 * 1024 * 1024),
        name="unpack",
    )(out, full)


def local(
    fine_points, parent, patch_count, qkv_fine, out_fine, pool_weight, qkv_coarse, out_coarse,
    cotangent,
):
    ab = fine_call(patch_count, parent.reshape(1, 1024), fine_points, qkv_fine, out_fine)
    sums, coarse_in, far_in, far_cot = middle_call(ab, pool_weight, cotangent)
    dn, mixed, big = coarse_call(coarse_in, far_in, cotangent, far_cot, qkv_coarse, out_coarse)
    return unpack_call(
        *tail_call(sums, pool_weight, coarse_in, cotangent, dn, mixed, out_coarse, big)
    )


def solution(mesh):
    rows = P(("rep", "pts"), None)
    flat = P(("rep", "pts"))
    return jax.shard_map(
        local,
        mesh=mesh,
        in_specs=(rows, flat, flat, P(), P(), P(), P(), P(), rows),
        out_specs=(rows, P(), P(), P(), P()),
        check_vma=False,
    )
```

```python
import jax
import jax.numpy as jnp
from jax import lax
from jax.experimental import pallas as pl
from jax.experimental.pallas import tpu as pltpu
from jax.sharding import PartitionSpec as P

F32 = jnp.float32
BF = jnp.bfloat16
EPS = 1e-6
LOG2E = 1.4426950408889634
LN2 = 0.6931471805599453
SAFE = 80.0
MESH = pl.DeviceIdType.MESH
VM = pl.BlockSpec(memory_space=pltpu.VMEM)
SM = pl.BlockSpec(memory_space=pltpu.SMEM)

NN = (((1,), (0,)), ((), ()))
NT = (((1,), (1,)), ((), ()))
TN = (((0,), (0,)), ((), ()))
TT = (((0,), (1,)), ((), ()))


def mm(a, b, dims=NN):
    return lax.dot_general(a, b, dims, preferred_element_type=F32)


def normalize(values):
    return values * lax.rsqrt(jnp.mean(values * values, axis=-1, keepdims=True) + EPS)


def split_dot(a, b):
    high = a.astype(BF)
    low = (a - high.astype(F32)).astype(BF)
    return mm(high, b) + mm(low, b)


def head_rows(rows, width):
    return lax.broadcasted_iota(jnp.int32, (rows, width), 0) // 16


def score_bound(qt, k):
    channels = qt.shape[0]
    heads = (
        lax.broadcasted_iota(jnp.int32, (channels, 128), 0) // 16
        == lax.broadcasted_iota(jnp.int32, (channels, 128), 1)
    ).astype(BF)
    kf = k.astype(F32)
    k2 = mm((kf * kf).astype(BF), heads)
    q = qt.astype(F32)
    q2 = (q * q).reshape(channels // 16, 16, qt.shape[1]).sum(axis=1)
    return jnp.max(q2) * jnp.max(k2)


def fine_kernel(
    cnt_ref, off_hbm, x_hbm, w_hbm, ow_hbm, ab_ref,
    k_ref, qt_ref, va_ref, mt_ref, off_ref, x_ref, w_ref, ow_ref, load,
):
    pairs = ((x_hbm, x_ref), (w_hbm, w_ref), (off_hbm, off_ref), (ow_hbm, ow_ref))
    loads = [pltpu.make_async_copy(a, b, load.at[i]) for i, (a, b) in enumerate(pairs)]
    for copy in loads:
        copy.start()
    count = cnt_ref[0]
    shift = (lax.axis_index("rep") * lax.axis_size("pts") + lax.axis_index("pts")) * 256
    loads[0].wait()
    x = x_ref[...]
    n = normalize(x.astype(F32)).astype(BF)
    loads[1].wait()
    loads[2].wait()
    loads[3].wait()
    offset = off_ref[...] - shift
    k_ref[...] = mm(n, w_ref[:, 256:512]).astype(BF)
    qt_ref[...] = (mm(w_ref[:, :256], n, TT) * (0.25 * LOG2E)).astype(BF)
    vt = mm(w_ref[:, 512:], n, TT).astype(BF)
    live = lax.broadcasted_iota(jnp.int32, (1, 1024), 1) < count
    ones = jnp.where(jnp.broadcast_to(live, (16, 1024)), 1.0, 0.0).astype(BF)
    for h in range(16):
        rows = vt[h * 16 : h * 16 + 16, :].astype(F32)
        va_ref[h, 0:16, :] = jnp.where(live, rows, 0.0).astype(BF)
        va_ref[h, 16:32, :] = ones
    bound = score_bound(qt_ref[...], k_ref[...])
    quick = bound < SAFE * SAFE

    def safe_head(h, carry):
        half = pl.multiple_of((h // 8) * 128, 128)
        row = pl.multiple_of(h * 16, 16)
        chosen = head_rows(128, 256) == h % 8
        alive = lax.broadcasted_iota(jnp.int32, (1024, 256), 0) < count
        for t in range(4):
            cols = slice(t * 256, t * 256 + 256)
            part = qt_ref[pl.ds(half, 128), cols]
            s = mm(k_ref[:, pl.ds(half, 128)], jnp.where(chosen, part, jnp.zeros_like(part)))
            s = jnp.where(alive, s, -1e30)
            s = s - jnp.max(s, axis=0, keepdims=True)
            o = mm(va_ref[h], jnp.exp2(s).astype(BF))
            mt_ref[pl.ds(row, 16), cols] = (o[:16] / o[16:]).astype(BF)
        return carry

    def quick_head(h, carry):
        half = pl.multiple_of((h // 8) * 128, 128)
        row = pl.multiple_of(h * 16, 16)
        ck, cq = 1024, 256
        units = [(t, c) for t in range(1024 // cq) for c in range(1024 // ck)]
        chosen = head_rows(128, cq) == h % 8
        scores, weights, sums, queries = {}, {}, {}, {}
        for i in range(len(units) + 2):
            if i < len(units):
                t, c = units[i]
                if c == 0:
                    part = qt_ref[pl.ds(half, 128), t * cq : t * cq + cq]
                    queries[t] = jnp.where(chosen, part, jnp.zeros_like(part))
                scores[i] = mm(k_ref[c * ck : c * ck + ck, pl.ds(half, 128)], queries[t])
            if 1 <= i <= len(units):
                weights[i - 1] = jnp.exp2(scores.pop(i - 1)).astype(BF)
            if i >= 2:
                t, c = units[i - 2]
                o = mm(va_ref[h, :, c * ck : c * ck + ck], weights.pop(i - 2))
                sums[t] = o if c == 0 else sums[t] + o
                if c == 1024 // ck - 1:
                    o = sums.pop(t)
                    mt_ref[pl.ds(row, 16), t * cq : t * cq + cq] = (o[:16] / o[16:]).astype(BF)
        return carry

    @pl.when(quick)
    def _():
        lax.fori_loop(0, 16, quick_head, 0, unroll=4)

    @pl.when(jnp.logical_not(quick))
    def _():
        lax.fori_loop(0, 16, safe_head, 0)

    table = jnp.where(
        (lax.broadcasted_iota(jnp.int32, (288, 1024), 0) == offset) & live, 1.0, 0.0
    )
    total = jnp.sum(table, axis=1, keepdims=True)
    table = table.astype(BF)
    b = mm(table, mt_ref[...], NT)
    ab_ref[:, :256] = mm(table, x) + split_dot(b, ow_ref[...])
    ab_ref[:, 256:512] = b
    ab_ref[:, 512:] = jnp.broadcast_to(total, (288, 128))


def fine_call(count, offset, x, w, ow):
    return pl.pallas_call(
        fine_kernel,
        out_shape=jax.ShapeDtypeStruct((288, 640), F32),
        in_specs=[SM] + [pl.BlockSpec(memory_space=pltpu.HBM)] * 4,
        out_specs=VM,
        scratch_shapes=[
            pltpu.VMEM((1024, 256), BF),
            pltpu.VMEM((256, 1024), BF),
            pltpu.VMEM((16, 32, 1024), BF),
            pltpu.VMEM((256, 1024), BF),
            pltpu.VMEM((1, 1024), jnp.int32),
            pltpu.VMEM((1024, 256), BF),
            pltpu.VMEM((256, 768), BF),
            pltpu.VMEM((256, 256), BF),
            pltpu.SemaphoreType.DMA((4,)),
        ],
        compiler_params=pltpu.CompilerParams(vmem_limit_bytes=54 * 1024 * 1024),
        cost_estimate=pl.CostEstimate(flops=20 * 10**9, bytes_accessed=3 * 10**6, transcendentals=16 * 10**6),
        name="fine",
    )(count, offset, x, w, ow)


GA = 0.7978845608028654
GB = 0.044715


def pooled_mean(sums, pw_ref):
    count = jnp.maximum(sums[:, 512:513], 1.0)
    return split_dot(sums[:, :256], pw_ref[...]) / count, count


def gelu(u):
    return 0.5 * u * (1.0 + jnp.tanh(GA * (u + GB * u * u * u)))


def middle_kernel(
    ab_ref, pw_ref, ct_ref, sum_ref, c_ref, cf_ref, ctf_ref, arrived, send, recv
):
    rep = lax.axis_index("rep")
    pts = lax.axis_index("pts")
    total = lax.axis_size("pts")
    ahead = (rep, (pts + 1) % total)
    behind = (rep, (pts + total - 1) % total)
    partner = (rep, pts + 1 - 2 * (pts % 2))
    barrier = pltpu.get_barrier_semaphore()
    for peer in (ahead, behind, partner):
        pl.semaphore_signal(barrier, inc=1, device_id=peer, device_id_type=MESH)
    own, _ = pooled_mean(ab_ref[32:256], pw_ref)
    sum_ref[32:] = ab_ref[32:256]
    c_ref[32:] = gelu(own).astype(BF)
    pl.semaphore_wait(barrier, 3)

    def push(i, src, dst, peer):
        copy = pltpu.make_async_remote_copy(
            src_ref=src, dst_ref=dst, send_sem=send.at[i], recv_sem=recv.at[i],
            device_id=peer, device_id_type=MESH,
        )
        copy.start()
        return copy

    moved = push(0, ab_ref.at[pl.ds(256, 32)], arrived, ahead)
    cot = push(1, ct_ref, ctf_ref, partner)
    rest = push(2, c_ref.at[pl.ds(32, 224)], cf_ref.at[pl.ds(32, 224)], partner)
    moved.wait()
    first = ab_ref[:32] + arrived[...]
    sum_ref[:32] = first
    u, _ = pooled_mean(first, pw_ref)
    c_ref[:32] = gelu(u).astype(BF)
    last = push(3, c_ref.at[pl.ds(0, 32)], cf_ref.at[pl.ds(0, 32)], partner)
    cot.wait()
    rest.wait()
    last.wait()


def middle_call(ab, pw, ct):
    half = jax.ShapeDtypeStruct((256, 512), BF)
    return pl.pallas_call(
        middle_kernel,
        out_shape=(jax.ShapeDtypeStruct((256, 640), F32), half, half, half),
        in_specs=[VM] * 3,
        out_specs=(VM,) * 4,
        scratch_shapes=[
            pltpu.VMEM((32, 640), F32),
            pltpu.SemaphoreType.DMA((4,)),
            pltpu.SemaphoreType.DMA((4,)),
        ],
        compiler_params=pltpu.CompilerParams(
            collective_id=1, has_side_effects=True, vmem_limit_bytes=12 * 1024 * 1024
        ),
        cost_estimate=pl.CostEstimate(flops=9 * 10**9, bytes_accessed=10**6, transcendentals=10**5),
        name="middle",
    )(ab, pw, ct)


def coarse_kernel(
    c_ref, cf_ref, ct_ref, ctf_ref, w_ref, ow_ref,
    dn_ref, mix_ref, g_ref,
    n_ref, cot_ref, k_ref, v_ref, kt_ref, qt_ref, va_ref, dot_ref, ot_ref, dp_ref,
    p_ref, pb_ref, ds_ref,
):
    core = lax.axis_index("pts") % 2
    lo = pl.multiple_of(core * 256, 256)
    n_ref[:256] = normalize(c_ref[...].astype(F32)).astype(BF)
    n_ref[256:] = normalize(cf_ref[...].astype(F32)).astype(BF)
    cot_ref[:256] = ct_ref[...]
    cot_ref[256:] = ctf_ref[...]
    n = n_ref[...]
    wq = w_ref[:, pl.ds(lo, 256)]
    wk = w_ref[:, pl.ds(512 + lo, 256)]
    wv = w_ref[:, pl.ds(1024 + lo, 256)]
    qt_ref[...] = (mm(wq, n, TT) * (0.25 * LOG2E)).astype(BF)
    k_ref[...] = mm(n, wk).astype(BF)
    v_ref[...] = mm(n, wv).astype(BF)
    kt_ref[...] = mm(wk, n, TT).astype(BF)
    vt = mm(wv, n, TT).astype(BF)
    for h in range(16):
        va_ref[h, :16, :] = vt[h * 16 : h * 16 + 16, :]
        va_ref[h, 16:, :] = jnp.ones((16, 512), BF)
    dot_ref[...] = mm(ow_ref[pl.ds(lo, 256), :], cot_ref[...], NT)
    quick = score_bound(qt_ref[...], k_ref[...]) < SAFE * SAFE

    def stage_one(h, slot, shift):
        half = pl.multiple_of((h // 8) * 128, 128)
        row = pl.multiple_of(h * 16, 16)
        chosen = head_rows(128, 512) == h % 8
        part = qt_ref[pl.ds(half, 128), :]
        qm = jnp.where(chosen, part, jnp.zeros_like(part))
        s = mm(k_ref[:, pl.ds(half, 128)], qm)
        if shift:
            s = s - jnp.max(s, axis=0, keepdims=True)
        p = jnp.exp2(s)
        p_ref[slot] = p
        pb_ref[slot] = p.astype(BF)

    def stage_two(h, slot):
        half = pl.multiple_of((h // 8) * 128, 128)
        row = pl.multiple_of(h * 16, 16)
        chosen = head_rows(128, 512) == h % 8
        pb = pb_ref[slot]
        o = mm(va_ref[h], pb)
        inverse = 1.0 / o[16:]
        on = o[:16] * inverse
        ot_ref[pl.ds(row, 16), :] = on.astype(BF)
        do = dot_ref[pl.ds(row, 16), :] * inverse
        dob = do.astype(BF)
        delta = jnp.sum(dob.astype(F32) * on, axis=0, keepdims=True)
        tiled = jnp.concatenate([dob] * 8, axis=0)
        dom = jnp.where(chosen, tiled, jnp.zeros_like(tiled))
        dpt = mm(v_ref[:, pl.ds(half, 128)], dom)
        ds_ref[slot] = (p_ref[slot] * (dpt - delta)).astype(BF)
        dp_ref[pl.ds(512 + row, 16), :] = mm(dob, pb, NT).astype(BF)

    def stage_three(h, slot):
        row = pl.multiple_of(h * 16, 16)
        ds = ds_ref[slot]
        dp_ref[pl.ds(row, 16), :] = (mm(kt_ref[pl.ds(row, 16), :], ds) * 0.25).astype(BF)
        dk = mm(qt_ref[pl.ds(row, 16), :], ds, NT) * LN2
        dp_ref[pl.ds(256 + row, 16), :] = dk.astype(BF)

    def attend(shift):
        stage_one(0, 0, shift)
        stage_one(1, 1, shift)
        stage_two(0, 0)

        def step(j, carry):
            for e in (0, 1):
                h = 2 * j + e
                stage_two(h + 1, 1 - e)
                stage_three(h, e)
                stage_one(h + 2, e, shift)
            return carry

        lax.fori_loop(0, 7, step, 0)
        stage_two(15, 1)
        stage_three(14, 0)
        stage_three(15, 1)

    @pl.when(quick)
    def _():
        attend(False)

    @pl.when(jnp.logical_not(quick))
    def _():
        attend(True)

    mix_ref[...] = jnp.transpose(ot_ref[...])
    dnt = (
        mm(wq, dp_ref[:256, :]) + mm(wk, dp_ref[256:512, :]) + mm(wv, dp_ref[512:, :])
    ).astype(BF)
    dn_ref[...] = jnp.transpose(dnt)
    nt = jnp.transpose(n_ref[...])
    for j in range(6):
        block = mm(nt, dp_ref[j * 128 : j * 128 + 128, :], NT).astype(BF)
        g_ref[j * 32 : j * 32 + 32] = block.reshape(32, 16, 128)
    for j in range(4):
        block = mm(ot_ref[...], cot_ref[:, j * 128 : j * 128 + 128]).astype(BF)
        g_ref[192 + j * 16 : 208 + j * 16] = block.reshape(16, 16, 128)


def coarse_call(c, cf, ct, ctf, w, ow):
    return pl.pallas_call(
        coarse_kernel,
        out_shape=(
            jax.ShapeDtypeStruct((512, 512), BF),
            jax.ShapeDtypeStruct((512, 256), BF),
            jax.ShapeDtypeStruct((256, 16, 128), BF),
        ),
        in_specs=[VM] * 6,
        out_specs=(VM, VM, VM),
        scratch_shapes=[
            pltpu.VMEM((512, 512), BF),
            pltpu.VMEM((512, 512), BF),
            pltpu.VMEM((512, 256), BF),
            pltpu.VMEM((512, 256), BF),
            pltpu.VMEM((256, 512), BF),
            pltpu.VMEM((256, 512), BF),
            pltpu.VMEM((16, 32, 512), BF),
            pltpu.VMEM((256, 512), F32),
            pltpu.VMEM((256, 512), BF),
            pltpu.VMEM((768, 512), BF),
            pltpu.VMEM((2, 512, 512), F32),
            pltpu.VMEM((2, 512, 512), BF),
            pltpu.VMEM((2, 512, 512), BF),
        ],
        compiler_params=pltpu.CompilerParams(vmem_limit_bytes=28 * 1024 * 1024),
        name="coarse",
    )(c, cf, ct, ctf, w, ow)


def other_one(v):
    return v + 1 - 2 * (v % 2)


def other_two(v):
    return 3 - v


def tail_kernel(
    ab_ref, pw_ref, c_ref, ct_ref, dn_ref, mix_ref, ow_ref, big,
    out_ref, full,
    dnf, mixf, slope_ref, at_ref, bt_ref, small, sm, g, r1, s1, r2, ra, rb,
    ha, hb, ra2, rb2, z, rz, zf, fa, fb, send, recv,
):
    rep = lax.axis_index("rep")
    pts = lax.axis_index("pts")
    x = rep % 4
    zlo = rep // 4
    y = pts // 8
    zhi = (pts // 2) % 4
    core = pts % 2
    zi = zhi * 2 + zlo

    def at_x(v):
        return (zlo * 4 + v, pts)

    def at_y(v):
        return (rep, v * 8 + zhi * 2 + core)

    def at_z(v):
        return ((v % 2) * 4 + x, y * 8 + (v // 2) * 2 + core)

    partner = (rep, pts + 1 - 2 * core)
    barrier = pltpu.get_barrier_semaphore()
    peers = [partner]
    peers += [at_x((x + d) % 4) for d in (1, 2, 3)] + [at_y((y + d) % 4) for d in (1, 2, 3)]
    peers += [at_z((zi + d) % 8) for d in range(1, 8)]
    for peer in peers:
        pl.semaphore_signal(barrier, inc=1, device_id=peer, device_id_type=MESH)
    c = c_ref[...].astype(F32)
    u, count = pooled_mean(ab_ref[...], pw_ref)
    th = jnp.tanh(GA * (u + GB * u * u * u))
    slope = 0.5 * (1.0 + th) + 0.5 * u * (1.0 - th * th) * (GA * (1.0 + 3.0 * GB * u * u))
    slope_ref[...] = slope / count
    r = lax.rsqrt(jnp.mean(c * c, axis=-1, keepdims=True) + EPS)
    at_ref[...] = jnp.transpose(ab_ref[:, :256]).astype(BF)
    bt_ref[...] = jnp.transpose(ab_ref[:, 256:512]).astype(BF)
    pl.semaphore_wait(barrier, len(peers))

    counter = [0]

    def push(src, dst, peer):
        i = counter[0]
        counter[0] += 1
        copy = pltpu.make_async_remote_copy(
            src_ref=src, dst_ref=dst, send_sem=send.at[i], recv_sem=recv.at[i],
            device_id=peer, device_id_type=MESH,
        )
        copy.start()
        return copy

    def share(rows, peer):
        spot = full.at[core, rows]
        return push(spot, spot, peer)

    def wait(copies):
        for copy in copies:
            copy.wait()

    def f32(value):
        return value.astype(F32)

    def add(own, slots):
        total = f32(own)
        for slot in slots:
            total = total + f32(slot)
        return total.astype(BF)

    def quarter(base, v):
        return pl.ds(base + v * 8, 8)

    third, done = [], []

    def chain(m):
        streams = [
            (x, at_x, m * 128, other_one, other_two),
            (x, at_x, m * 128 + 32, other_two, other_one),
            (y, at_y, m * 128 + 64, other_one, other_two),
            (y, at_y, m * 128 + 96, other_two, other_one),
        ]
        n = 4 + 2 * m
        w = 1 + m
        some = pl.ds(0, n)
        few = pl.ds(0, w)
        first = []
        for k, (v, place, base, one, two) in enumerate(streams):
            p = one(v)
            first.append(push(big.at[quarter(base, two(p))], r1.at[m, k, 1], place(p)))
            first.append(push(big.at[quarter(base, p)], r1.at[m, k, 0], place(p)))
        yield
        second = []
        for k, (v, place, base, one, two) in enumerate(streams):
            wait(first[2 * k : 2 * k + 2])
            s1[m, k] = add(big[quarter(base, two(v))], [r1[m, k, 1]])
            second.append(push(s1.at[m, k], r2.at[m, k], place(two(v))))
        yield
        for k, (v, place, base, one, two) in enumerate(streams):
            second[k].wait()
            total = add(big[quarter(base, v)], [r1[m, k, 0], r2[m, k]])
            keep = ha if k < 2 else hb
            spot = (k % 2) * 2
            keep[m, :, spot : spot + 2] = total.reshape(4, 2, 16, 128)
        if m:
            wait(third)
            total = add(g[pl.ds(x * 8, 8)], [ra[d] for d in range(3)])
            ha[m, :, 4:] = total.reshape(4, 2, 16, 128)
            total = add(g[pl.ds(32 + y * 8, 8)], [rb[d] for d in range(3)])
            hb[m, :, 4:] = total.reshape(4, 2, 16, 128)
        moves = []
        for d in (2, 1, 3):
            to = (y + d) % 4
            moves.append(push(ha.at[m, to, some], ra2.at[m, d - 1, some], at_y(to)))
            to = (x + d) % 4
            moves.append(push(hb.at[m, to, some], rb2.at[m, d - 1, some], at_x(to)))
        yield
        wait(moves)
        z[m, :n] = add(ha[m, y, :n], [ra2[m, d, :n] for d in range(3)])
        z[m, n : 2 * n] = add(hb[m, x, :n], [rb2[m, d, :n] for d in range(3)])
        if m:
            z[m, 12:] = jnp.zeros((4, 16, 128), BF)
        moves = []
        for d in (4, 3, 5, 2, 6, 1, 7):
            to = (zi + d) % 8
            moves.append(push(z.at[m, pl.ds(to * w, w)], rz.at[m, d - 1, few], at_z(to)))
        yield
        wait(moves)
        mine = pl.ds(zi * w, w)
        zf[m, mine] = add(z[m, mine], [rz[m, d, :w] for d in range(7)])
        spot = zf.at[m, mine]
        moves = [push(spot, spot, at_z((zi + d) % 8)) for d in (4, 3, 5, 2, 6, 1, 7)]
        yield
        wait(moves)
        fa[m, y, :n] = zf[m, :n]
        fb[m, x, :n] = zf[m, n : 2 * n]
        moves = []
        for d in (2, 1, 3):
            spot = fa.at[m, y, some]
            moves.append(push(spot, spot, at_y((y + d) % 4)))
            spot = fb.at[m, x, some]
            moves.append(push(spot, spot, at_x((x + d) % 4)))
        yield
        wait(moves)
        first, second, ups = [], [], []
        for k, (v, place, base, one, two) in enumerate(streams):
            kept = fa if k < 2 else fb
            spot = (k % 2) * 2
            own = quarter(base, v)
            full[core, own] = kept[m, :, spot : spot + 2].reshape(8, 16, 128)
            first.append(share(own, place(two(v))))
            second.append(share(own, place(one(v))))
            done.append(share(own, partner))
        if m:
            la, lb = pl.ds(256 + x * 8, 8), pl.ds(288 + y * 8, 8)
            full[core, la] = fa[m, :, 4:].reshape(8, 16, 128)
            full[core, lb] = fb[m, :, 4:].reshape(8, 16, 128)
            for d in (2, 1, 3):
                ups.append(share(la, at_x((x + d) % 4)))
                ups.append(share(lb, at_y((y + d) % 4)))
        yield
        for k, (v, place, base, one, two) in enumerate(streams):
            first[k].wait()
            came = quarter(base, two(v))
            second.append(share(came, place(one(v))))
            done.append(share(came, partner))
        yield
        if m:
            wait(ups)
            done.append(share(pl.ds(256, 48), partner))
        for k, (v, place, base, one, two) in enumerate(streams):
            second[k].wait()
            second[4 + k].wait()
            done.append(share(quarter(base, one(v)), partner))
            done.append(share(quarter(base, two(one(v))), partner))

    trade = [push(dn_ref.at[pl.ds(256, 256)], dnf, partner)]
    trade.append(push(mix_ref.at[pl.ds(256, 256)], mixf, partner))
    halves = [chain(0), chain(1)]
    next(halves[0])
    next(halves[1])
    wait(trade)
    dn = f32(dn_ref[:256]) + f32(dnf[...])
    inner = jnp.mean(dn * c, axis=-1, keepdims=True)
    dc = r * dn - c * (r * r * r * inner) + f32(ct_ref[...])
    gs = (slope_ref[...] * dc).astype(BF)
    gw = mm(gs, pw_ref[...], NT).astype(BF)
    for half in range(2):
        rows = slice(half * 128, half * 128 + 128)
        for j in range(4):
            block = mm(at_ref[rows], gs[:, j * 128 : j * 128 + 128]).astype(BF)
            small[half, j * 8 : j * 8 + 8] = block.reshape(8, 16, 128)
        for j in range(2):
            block = mm(bt_ref[rows], gw[:, j * 128 : j * 128 + 128]).astype(BF)
            small[half, 32 + j * 8 : 40 + j * 8] = block.reshape(8, 16, 128)
    swap = push(small.at[1 - core], sm, partner)
    next(halves[0])
    swap.wait()
    g[:48] = add(small[core], [sm[...]])
    g[48:] = jnp.zeros((16, 16, 128), BF)
    next(halves[1])
    for d in (2, 1, 3):
        to = (x + d) % 4
        third.append(push(g.at[pl.ds(to * 8, 8)], ra.at[d - 1], at_x(to)))
        to = (y + d) % 4
        third.append(push(g.at[pl.ds(32 + to * 8, 8)], rb.at[d - 1], at_y(to)))
    next(halves[0])
    lo = pl.multiple_of(core * 256, 256)
    hi = pl.multiple_of(256 - core * 256, 256)
    mixed = mm(mix_ref[:256], ow_ref[pl.ds(lo, 256), :]) + mm(mixf[...], ow_ref[pl.ds(hi, 256), :])
    out_ref[...] = (f32(c_ref[...]) + mixed).astype(BF)
    next(halves[1])
    for _ in range(7):
        for half in halves:
            next(half, None)
    wait(done)


def unpack_kernel(out_ref, full, copy_ref, gof_ref, gp_ref, gq_ref, goc_ref):
    copy_ref[...] = out_ref[...]
    for c in range(2):
        for j in range(6):
            column = (j // 2) * 512 + c * 256 + (j % 2) * 128
            gq_ref[:, column : column + 128] = full[c, j * 32 : j * 32 + 32].reshape(512, 128)
        for j in range(4):
            rows = slice(c * 256, c * 256 + 256)
            tile = full[c, 192 + j * 16 : 208 + j * 16].reshape(256, 128)
            goc_ref[rows, j * 128 : j * 128 + 128] = tile
        rows = slice(c * 128, c * 128 + 128)
        for j in range(4):
            tile = full[c, 256 + j * 8 : 264 + j * 8].reshape(128, 128)
            gp_ref[rows, j * 128 : j * 128 + 128] = tile
        for j in range(2):
            tile = full[c, 288 + j * 8 : 296 + j * 8].reshape(128, 128)
            gof_ref[rows, j * 128 : j * 128 + 128] = tile


def tail_call(*operands):
    def tiles(*n):
        return pltpu.VMEM((*n, 16, 128), BF)

    return pl.pallas_call(
        tail_kernel,
        out_shape=(
            jax.ShapeDtypeStruct((256, 512), BF),
            jax.ShapeDtypeStruct((2, 320, 16, 128), BF),
        ),
        in_specs=[VM] * 8,
        out_specs=(VM,) * 2,
        scratch_shapes=[
            pltpu.VMEM((256, 512), BF), pltpu.VMEM((256, 256), BF),
            pltpu.VMEM((256, 512), F32), pltpu.VMEM((256, 256), BF), pltpu.VMEM((256, 256), BF),
            tiles(2, 48), tiles(48), tiles(64),
            tiles(2, 4, 2, 8), tiles(2, 4, 8), tiles(2, 4, 8), tiles(3, 8), tiles(3, 8),
            tiles(2, 4, 6), tiles(2, 4, 6), tiles(2, 3, 6), tiles(2, 3, 6),
            tiles(2, 16), tiles(2, 7, 2), tiles(2, 16), tiles(2, 4, 6), tiles(2, 4, 6),
            pltpu.SemaphoreType.DMA((150,)),
            pltpu.SemaphoreType.DMA((150,)),
        ],
        compiler_params=pltpu.CompilerParams(
            collective_id=0, has_side_effects=True, vmem_limit_bytes=20 * 1024 * 1024
        ),
        name="tail",
    )(*operands)


def unpack_call(out, full):
    return pl.pallas_call(
        unpack_kernel,
        out_shape=(
            jax.ShapeDtypeStruct((256, 512), BF),
            jax.ShapeDtypeStruct((256, 256), BF),
            jax.ShapeDtypeStruct((256, 512), BF),
            jax.ShapeDtypeStruct((512, 1536), BF),
            jax.ShapeDtypeStruct((512, 512), BF),
        ),
        in_specs=[VM] * 2,
        out_specs=(VM,) * 5,
        compiler_params=pltpu.CompilerParams(vmem_limit_bytes=12 * 1024 * 1024),
        name="unpack",
    )(out, full)


def local(
    fine_points, parent, patch_count, qkv_fine, out_fine, pool_weight, qkv_coarse, out_coarse,
    cotangent,
):
    ab = fine_call(patch_count, parent.reshape(1, 1024), fine_points, qkv_fine, out_fine)
    sums, coarse_in, far_in, far_cot = middle_call(ab, pool_weight, cotangent)
    dn, mixed, big = coarse_call(coarse_in, far_in, cotangent, far_cot, qkv_coarse, out_coarse)
    return unpack_call(
        *tail_call(sums, pool_weight, coarse_in, cotangent, dn, mixed, out_coarse, big)
    )


def solution(mesh):
    rows = P(("rep", "pts"), None)
    flat = P(("rep", "pts"))
    return jax.shard_map(
        local,
        mesh=mesh,
        in_specs=(rows, flat, flat, P(), P(), P(), P(), P(), rows),
        out_specs=(rows, P(), P(), P(), P()),
        check_vma=False,
    )
```
